512 devices in a mesh: vocab: 32 (over x, z_lo, core), batch: 16 (over y, z_hi).
Axes of the slice: x: 4, y: 4, z: 16 (z_hi: 4, z_lo: 4; z = z_hi * 4 + z_lo), core: 2. Of those that a mesh axis runs over, the one named last changes fastest.
Arguments:
- neighbour_ids: int32 [512, 128], P(('vocab', 'batch')), may hold values from 0 to 127999, as said below
- query_states: bfloat16 [256, 64, 4096], P('vocab', None, 'batch'), may hold values from -6 to 6
- table: bfloat16 [128000, 4096], P('vocab', 'batch'), may hold values from -6 to 6
- in_proj: bfloat16 [4096, 896], P('batch'), may hold values from -0.09375 to 0.09375
- kv_proj: bfloat16 [4096, 896], P('batch'), may hold values from -0.09375 to 0.09375
- norm_self: float32 [896], replicated, may hold values from 0.25 to 1.75
- self_qkv: bfloat16 [896, 1344], P('batch'), may hold values from -0.1875 to 0.1875
- self_out: bfloat16 [448, 896], P('batch'), may hold values from -0.25 to 0.25
- norm_cross: float32 [896], replicated, may hold values from 0.25 to 1.75
- cross_q: bfloat16 [896, 448], P('batch'), may hold values from -0.1875 to 0.1875
- cross_out: bfloat16 [448, 896], P('batch'), may hold values from -0.25 to 0.25
Outputs:
- encoded: bfloat16 [512, 128, 896], P(('vocab', 'batch'))
The draws below stay inside these ranges and needn't reach their ends.
Inputs may be any that keep to these rules, and one draw needn't show every extreme that they name: `neighbour_ids`: ids fall in 32 consecutive blocks of 4000 ids; of one device's 1 * 128 tokens (rows of one device), at most 4 lie in one block, and in every such group some block holds exactly 4.
All inputs are finite; a program needn't handle non-finite values.
Results may differ from the reference program's by a relative error of at most 0.019.
Values may be sent and summed in bfloat16 or wider, within the bound.
A program may use at most 64 MiB of HBM per device.

```python
import jax
import jax.numpy as jnp
from jax import lax

D = 4096
DE = 896
VOCAB = 128000
HEADS = 7
HEAD = 64
R = 128
K = 2
QLEN = 64
NB_DEV = 1
NEIGH = 512
SPANS = 256
VOCAB_ROWS = 4000
CAP = 4
N_BATCH = 16


def draw_neighbour_ids(key, part):
    blocks_total = VOCAB // VOCAB_ROWS
    tokens = NB_DEV * R
    slots = blocks_total * CAP
    groups = NEIGH // NB_DEV

    def one_group(group_key):
        first_key, score_key, order_key, offset_key = jax.random.split(group_key, 4)
        slot_owner = jnp.arange(slots, dtype=jnp.int32) // CAP
        favoured = jax.random.randint(first_key, (), 0, blocks_total, dtype=jnp.int32)
        scores = jax.random.randint(score_key, (slots,), 0, 1024, dtype=jnp.int32) * slots + jnp.arange(slots, dtype=jnp.int32)
        scores = jnp.where(slot_owner == favoured, jnp.arange(slots, dtype=jnp.int32) - slots, scores)
        order = jnp.argsort(scores, stable=True)
        chosen = jnp.take(slot_owner, order)[:tokens]
        chosen = jax.random.permutation(order_key, chosen)
        offsets = jax.random.randint(offset_key, (tokens,), 0, VOCAB_ROWS, dtype=jnp.int32)
        return (chosen * VOCAB_ROWS + offsets).reshape(NB_DEV, R)
    group_keys = jax.random.split(jax.random.fold_in(key, 7), groups)
    return jax.vmap(one_group)(group_keys).reshape(NEIGH, R)


def level_of(own_key, dims, shards, smallest, top_value):
    level, own = 1.0, jax.random.fold_in(own_key, 6)
    for position, blocks in shards:
        draws = jnp.exp(jax.random.uniform(jax.random.fold_in(own, position), (blocks,), jnp.float32, smallest / len(shards), top_value / len(shards)))
        level = level * jnp.repeat(draws, dims[position] // blocks).reshape([-1 if axis == position else 1 for axis in range(len(dims))])
    return level


def noise(rng, dims, deviation, bound, cuts=(), kind=jnp.bfloat16):
    level = level_of(rng, dims, cuts, -0.22, 0.18) if cuts else 1.0
    result = jax.random.normal(rng, dims, jnp.float32) * deviation * level
    return jnp.minimum(jnp.maximum(result, -bound), bound).astype(kind)


def setup_inputs(seed: int = 0) -> dict:
    splits = jax.random.split(jax.random.key(seed), 12)
    return {
        "neighbour_ids": draw_neighbour_ids(jax.random.fold_in(splits[11], 71), 0),
        "query_states": noise(splits[1], (SPANS, QLEN, D), 1.0, 6.0, ((0, 32), (2, 16))),
        "table": noise(splits[2], (VOCAB, D), 1.0, 6.0, ((0, 32), (1, 16))),
        "in_proj": noise(splits[3], (D, DE), D ** -0.5, 0.09375, ((0, 16),)),
        "kv_proj": noise(splits[4], (D, 2 * HEADS * HEAD), D ** -0.5, 0.09375, ((0, 16),)),
        "norm_self": jnp.clip(1.0 + 0.15 * jax.random.normal(splits[5], (DE,), jnp.float32), 0.25, 1.75),
        "self_qkv": noise(splits[6], (DE, 3 * HEADS * HEAD), DE ** -0.5, 0.1875, ((0, 16),)),
        "self_out": noise(splits[7], (HEADS * HEAD, DE), (HEADS * HEAD) ** -0.5, 0.25, ((0, 16),)),
        "norm_cross": jnp.clip(1.0 + 0.15 * jax.random.normal(splits[8], (DE,), jnp.float32), 0.25, 1.75),
        "cross_q": noise(splits[9], (DE, HEADS * HEAD), DE ** -0.5, 0.1875, ((0, 16),)),
        "cross_out": noise(splits[10], (HEADS * HEAD, DE), (HEADS * HEAD) ** -0.5, 0.25, ((0, 16),)),
    }


def norm_rows(values, gain):
    scale = lax.rsqrt(lax.optimization_barrier(jnp.mean(values * values, axis=-1, keepdims=True)) + 1e-06)
    return values * scale * gain.astype(jnp.float32)

def attend(queries, keys, values):
    scores = jnp.einsum('nahd,nbhd->nhab', queries.astype(jnp.float32), keys.astype(jnp.float32)) * HEAD ** (-0.5)
    weights = jax.nn.softmax(scores, axis=-1).astype(jnp.bfloat16)
    return jnp.einsum('nhab,nbhd->nahd', weights.astype(jnp.float32), values.astype(jnp.float32)).astype(jnp.bfloat16)

def encode(start_rows, span_kv, norm_self, self_qkv, self_out, norm_cross, cross_q, cross_out):
    count = start_rows.shape[0]
    inner = HEADS * HEAD
    stream = start_rows.astype(jnp.float32)
    self_in = norm_rows(stream, norm_self).astype(jnp.bfloat16)
    mixed = jnp.einsum('nrd,de->nre', self_in.astype(jnp.float32), self_qkv.astype(jnp.float32)).astype(jnp.bfloat16)
    queries = mixed[:, :, :inner].reshape(count, R, HEADS, HEAD)
    keys = mixed[:, :, inner:2 * inner].reshape(count, R, HEADS, HEAD)
    values = mixed[:, :, 2 * inner:].reshape(count, R, HEADS, HEAD)
    self_heads = attend(queries, keys, values).reshape(count, R, inner)
    stream = stream + jnp.einsum('nre,ed->nrd', self_heads.astype(jnp.float32), self_out.astype(jnp.float32))
    cross_in = norm_rows(stream, norm_cross).astype(jnp.bfloat16)
    cross_query = jnp.einsum('nrd,de->nre', cross_in.astype(jnp.float32), cross_q.astype(jnp.float32)).astype(jnp.bfloat16)
    cross_keys = span_kv[:, :, :inner].reshape(count, QLEN, HEADS, HEAD)
    cross_values = span_kv[:, :, inner:].reshape(count, QLEN, HEADS, HEAD)
    cross_heads = attend(cross_query.reshape(count, R, HEADS, HEAD), cross_keys, cross_values).reshape(count, R, inner)
    stream = stream + jnp.einsum('nre,ed->nrd', cross_heads.astype(jnp.float32), cross_out.astype(jnp.float32))
    return stream.astype(jnp.bfloat16)

def reference(neighbour_ids, query_states, table, in_proj, kv_proj, norm_self, self_qkv, self_out, norm_cross, cross_q, cross_out):
    inner = HEADS * HEAD
    width = D // N_BATCH
    pair_sum = jnp.zeros((SPANS, QLEN, 2 * inner), jnp.float32)
    for column in range(N_BATCH):
        states_part = query_states[:, :, column * width:(column + 1) * width].astype(jnp.float32)
        weight_part = kv_proj[column * width:(column + 1) * width].astype(jnp.float32)
        term = jnp.einsum('cqd,de->cqe', states_part, weight_part).astype(jnp.bfloat16)
        term = lax.optimization_barrier(term)
        pair_sum = pair_sum + term.astype(jnp.float32)
    span_kv = pair_sum.astype(jnp.bfloat16)
    block = 16
    groups = NEIGH // block
    id_blocks = neighbour_ids.reshape(groups, block, R)
    firsts = jnp.arange(groups, dtype=jnp.int32) * block

    def one_block(pieces):
        ids_here, first = pieces
        embedded = jnp.take(table, ids_here, axis=0)
        start_sum = jnp.zeros((block, R, DE), jnp.float32)
        for column in range(N_BATCH):
            rows_part = embedded[:, :, column * width:(column + 1) * width].astype(jnp.float32)
            weight_part = in_proj[column * width:(column + 1) * width].astype(jnp.float32)
            term = jnp.einsum('nrd,de->nre', rows_part, weight_part).astype(jnp.bfloat16)
            term = lax.optimization_barrier(term)
            start_sum = start_sum + term.astype(jnp.float32)
        start_rows = start_sum.astype(jnp.bfloat16)
        span_index = (first + jnp.arange(block, dtype=jnp.int32)) // K
        span_here = jnp.take(span_kv, span_index, axis=0)
        return encode(start_rows, span_here, norm_self, self_qkv, self_out, norm_cross, cross_q, cross_out)
    encoded = lax.map(one_block, (id_blocks, firsts))
    return encoded.reshape(NEIGH, R, DE)
```

```python
import functools

import jax
import jax.numpy as jnp
from jax import lax
from jax.experimental import pallas as pl
from jax.experimental.pallas import tpu as pltpu
from jax.sharding import PartitionSpec as P

MESH = pl.DeviceIdType.MESH
BF = jnp.bfloat16
F32 = jnp.float32
HEAD = 64
NV = 32
NB = 16
QK_AT, V_AT, CQ_AT, SO_AT, CO_AT = 0, 56, 84, 112, 140
PIECE = 24
VMEM_LIMIT = 60 * 1024 * 1024


def where_am_i():
    v = lax.axis_index("vocab")
    b = lax.axis_index("batch")
    return v, b, v // 8, lax.rem(v, 2), b // 4, lax.rem(b, 4)


def send(src, dst, ssem, rsem, dev):
    return pltpu.make_async_remote_copy(
        src_ref=src, dst_ref=dst, send_sem=ssem, recv_sem=rsem,
        device_id=dev, device_id_type=MESH,
    )


def greet(v, b, all_batch):
    barrier = pltpu.get_barrier_semaphore()

    def hello_vocab(o, _):
        pl.semaphore_signal(
            barrier, inc=1, device_id=(lax.rem(v + o, NV), b), device_id_type=MESH
        )
        return 0

    lax.fori_loop(1, NV, hello_vocab, 0)
    if all_batch:
        def hello_batch(o, _):
            pl.semaphore_signal(
                barrier, inc=1, device_id=(v, lax.rem(b + o, NB)), device_id_type=MESH
            )
            return 0

        lax.fori_loop(1, NB, hello_batch, 0)
        pl.semaphore_wait(barrier, NV - 1 + NB - 1)
    else:
        y, z = b // 4, lax.rem(b, 4)
        for dy, dz in ((1, 0), (3, 0), (0, 1), (0, 3)):
            peer = lax.rem(y + dy, 4) * 4 + lax.rem(z + dz, 4)
            pl.semaphore_signal(barrier, inc=1, device_id=(v, peer), device_id_type=MESH)
        pl.semaphore_wait(barrier, NV - 1 + 4)


class RingSum:
    def __init__(self, chunk, got, ssem, rsem, ahead, behind):
        def m(i, src, dev):
            return send(src, got.at[i], ssem.at[i], rsem.at[i], dev)

        self.chunk, self.got = chunk, got
        self.opp_a = m(0, chunk(2, 0), ahead)
        self.opp_b = m(1, chunk(2, 1), behind)
        self.next_b = m(2, chunk(1, 1), ahead)
        self.prev_a = m(3, chunk(3, 0), behind)
        self.merged_a = m(4, chunk(1, 0), ahead)
        self.merged_b = m(5, chunk(3, 1), behind)

    def merge_a(self):
        self.opp_a.wait_recv()
        ref = self.chunk(1, 0)
        ref[...] = (ref[...].astype(F32) + self.got[0].astype(F32)).astype(BF)
        self.merged_a.start()

    def merge_b(self):
        self.opp_b.wait_recv()
        ref = self.chunk(3, 1)
        ref[...] = (ref[...].astype(F32) + self.got[1].astype(F32)).astype(BF)
        self.merged_b.start()

    def total(self):
        self.prev_a.wait_recv()
        self.merged_a.wait_recv()
        a = self.chunk(0, 0)[...].astype(F32) + self.got[3].astype(F32) + self.got[4].astype(F32)
        self.next_b.wait_recv()
        self.merged_b.wait_recv()
        b = self.chunk(0, 1)[...].astype(F32) + self.got[2].astype(F32) + self.got[5].astype(F32)
        return a, b

    def drain(self):
        for c in (self.opp_a, self.opp_b, self.next_b, self.prev_a, self.merged_a, self.merged_b):
            c.wait_send()


class RingCopies:
    def __init__(self, own, slot, half, me, ssem, rsem, ahead, behind):
        left, right = lax.rem(me + 3, 4), lax.rem(me + 1, 4)
        far = lax.rem(me + 2, 4)
        self.to_ahead = send(own, slot(me), ssem.at[0], rsem.at[0], ahead)
        self.to_behind = send(own, slot(me), ssem.at[1], rsem.at[1], behind)
        self.on_ahead = send(half(left, 0), half(left, 0), ssem.at[2], rsem.at[2], ahead)
        self.on_behind = send(half(right, 1), half(right, 1), ssem.at[3], rsem.at[3], behind)
        self.from_left = (slot(left), rsem.at[0])
        self.from_right = (slot(right), rsem.at[1])
        self.far_a = (half(far, 0), rsem.at[2])
        self.far_b = (half(far, 1), rsem.at[3])

    def start(self):
        self.to_ahead.start()
        self.to_behind.start()

    def forward(self):
        self.to_ahead.wait_recv()
        self.on_ahead.start()
        self.to_behind.wait_recv()
        self.on_behind.start()

    def finish(self):
        self.on_ahead.wait_recv()
        self.on_behind.wait_recv()

    def drain(self):
        for c in (self.to_ahead, self.to_behind, self.on_ahead, self.on_behind):
            c.wait_send()


def packed_rows(start, count):
    done = 0
    while done < count:
        at = start + done
        take = min(count - done, PIECE - at % PIECE)
        yield done, at // PIECE, at % PIECE, take
        done += take


def first_kernel(
    ids_ref, q_ref, kvp_ref, qkv_ref, so_ref, cq_ref, co_ref,
    wanted_ref, span_ref, wg_out_ref,
    ids_got, row_ref, rows_got, pack, wg, kv_chunk, kv_got, kv_y, kv_in,
    ids_s, ids_r, row_s, row_r, wz_s, wz_r, wy_s, wy_r, ky_s, ky_r, kz_s, kz_r,
):
    v, b, x, c, y, z = where_am_i()
    greet(v, b, True)

    def ask(o, _):
        to = lax.rem(v + o, NV)
        send(ids_ref.at[to], ids_got.at[v], ids_s.at[o], ids_r.at[o], (to, b)).start()
        return 0

    lax.fori_loop(1, NV, ask, 0)

    def put(block, start, lanes):
        for at, piece, row, take in packed_rows(start, block.shape[0]):
            pack[piece, row : row + take, lanes] = block[at : at + take]

    whole = slice(0, 896)
    put(qkv_ref[:, 0:896], QK_AT, whole)
    put(jnp.concatenate([qkv_ref[0:28, 896:1344], qkv_ref[28:56, 896:1344]], axis=1), V_AT, whole)
    put(jnp.concatenate([cq_ref[0:28, :], cq_ref[28:56, :]], axis=1), CQ_AT, whole)
    put(so_ref[...], SO_AT, whole)
    put(co_ref[...], CO_AT, whole)
    pack[7] = jnp.zeros_like(pack[7])
    member = x * 2 + c
    wz = []
    for o in (2, 1, 3):
        wz.append(
            send(pack.at[member], wg.at[y, z], wz_s.at[o - 1], wz_r.at[o - 1],
                 (v, y * 4 + lax.rem(z + o, 4)))
        )
        wz[-1].start()
    wg[y, z] = pack[member]

    ahead = (v, lax.rem(y + 1, 4) * 4 + z)
    behind = (v, lax.rem(y + 3, 4) * 4 + z)
    ky = RingSum(lambda r, h: kv_chunk.at[r, h], kv_got, ky_s, ky_r, ahead, behind)
    for r in (2, 1, 3, 0):
        term = jnp.dot(q_ref[lax.rem(y + r, 4)], kvp_ref[...], preferred_element_type=F32)
        kv_chunk[r] = term.reshape(2, 64, 896).astype(BF)
        if r == 2:
            ky.opp_a.start()
            ky.opp_b.start()
        elif r == 1:
            ky.next_b.start()
        elif r == 3:
            ky.prev_a.start()

    def asked(o, _):
        send(ids_ref.at[v], ids_got.at[v], ids_s.at[o], ids_r.at[o], (v, b)).wait_recv()
        return 0

    lax.fori_loop(1, NV, asked, 0)
    ids_got[v] = ids_ref[v]
    row_ref[...] = jnp.sum(ids_got[...], axis=0)

    def tell(o, _):
        to = lax.rem(b + o, NB)
        send(row_ref, rows_got.at[b], row_s.at[o], row_r.at[o], (v, to)).start()
        return 0

    lax.fori_loop(1, NB, tell, 0)
    rows_got[b] = row_ref[...]

    ky.merge_a()
    ky.merge_b()
    for copy in wz:
        copy.wait_recv()
    wy = RingCopies(
        wg.at[y], lambda i: wg.at[i], lambda i, h: wg.at[i, pl.ds(2 * h, 2)], y, wy_s, wy_r, ahead, behind
    )
    wy.start()
    a, bb = ky.total()
    kv_y[0] = a.astype(BF)
    kv_y[1] = bb.astype(BF)
    mine = z // 2
    odd = lax.rem(z, 2)
    outside = (v, y * 4 + lax.rem(z + 3 + 2 * odd, 4))
    kz = send(kv_y.at[1 - mine], kv_in, kz_s, kz_r, outside)
    kz.start()
    wy.forward()

    def told(o, _):
        send(row_ref, rows_got.at[b], row_s.at[o], row_r.at[o], (v, b)).wait_recv()
        return 0

    lax.fori_loop(1, NB, told, 0)
    wanted_ref[...] = rows_got[:, 0, :]
    kz.wait_recv()
    span_ref[...] = (kv_y[mine].astype(F32) + kv_in[...].astype(F32)).astype(BF)
    wy.finish()
    for i in range(4):
        wg_out_ref[pl.ds(4 * i, 4)] = wg[i]

    def sent_ids(o, _):
        send(ids_ref.at[v], ids_got.at[v], ids_s.at[o], ids_r.at[o], (v, b)).wait_send()
        return 0

    lax.fori_loop(1, NV, sent_ids, 0)

    def sent_rows(o, _):
        send(row_ref, rows_got.at[b], row_s.at[o], row_r.at[o], (v, b)).wait_send()
        return 0

    lax.fori_loop(1, NB, sent_rows, 0)
    for copy in wz:
        copy.wait_send()
    wy.drain()
    ky.drain()
    kz.wait_send()


def normed(values, gain):
    scale = lax.rsqrt(jnp.mean(values * values, axis=-1, keepdims=True) + 1e-06)
    return (values * scale * gain).astype(BF)


def softmax(scores):
    e = jnp.exp(scores - jnp.max(scores, axis=-1, keepdims=True))
    return (e / jnp.sum(e, axis=-1, keepdims=True)).astype(BF)


def attend(queries, keys, values):
    outs = []
    for h in range(queries.shape[1] // HEAD):
        cut = slice(h * HEAD, (h + 1) * HEAD)
        scores = lax.dot_general(
            queries[:, cut], keys[:, cut], (((1,), (1,)), ((), ())), preferred_element_type=F32
        ) * HEAD ** (-0.5)
        outs.append(jnp.dot(softmax(scores), values[:, cut], preferred_element_type=F32).astype(BF))
    return jnp.concatenate(outs, axis=1)


def second_kernel(
    looked_ref, inp_ref, sel_ref, span_ref, wg_ref, ns_ref, nc_ref,
    out_ref,
    chunk, y_got, z_chunk, z_got, sums, back_out, back_in, back_rows, full, mate_span,
    w_qk, w_v, w_cq, w_so, w_co,
    y_s, y_r, z_s, z_r, back_s, back_r, wx_s, wx_r, wc_s, wc_r, m_s, m_r,
):
    v, b, x, c, y, z = where_am_i()
    greet(v, b, False)
    ahead = (v, lax.rem(y + 1, 4) * 4 + z)
    behind = (v, lax.rem(y + 3, 4) * 4 + z)
    z_ahead = (v, y * 4 + lax.rem(z + 1, 4))
    z_behind = (v, y * 4 + lax.rem(z + 3, 4))
    rest = lax.rem(v, 8)
    x_ahead = (lax.rem(x + 1, 4) * 8 + rest, b)
    x_behind = (lax.rem(x + 3, 4) * 8 + rest, b)
    odd = lax.rem(z, 2)
    z_mate = (v, y * 4 + z + 1 - 2 * odd)
    mate = (v + 1 - 2 * c, b)

    spans = send(span_ref, mate_span, m_s, m_r, z_mate)
    spans.start()
    wx = RingCopies(
        wg_ref, lambda i: full.at[c, i], lambda i, h: full.at[c, i, pl.ds(8 * h, 8)], x,
        wx_s, wx_r, x_ahead, x_behind,
    )
    wx.start()

    order = (2, 1, 3, 0)
    sums_y = []
    for k, rz in enumerate(order):
        ring = RingSum(
            lambda r, h, k=k: chunk.at[k, r, h], y_got.at[k], y_s.at[k], y_r.at[k], ahead, behind
        )
        sums_y.append(ring)
        for r in order:
            peer = lax.rem(y + r, 4) * 4 + lax.rem(z + rz, 4)
            term = jnp.dot(looked_ref[peer], inp_ref[...], preferred_element_type=F32)
            chunk[k, r] = term.reshape(2, 64, 896).astype(BF)
            if r == 2:
                ring.opp_a.start()
                ring.opp_b.start()
            elif r == 1:
                ring.next_b.start()
            elif r == 3:
                ring.prev_a.start()

    to_mate = []

    def pass_on(i, src, dst):
        copy = send(src, dst, wc_s.at[i], wc_r.at[i], mate)
        copy.start()
        to_mate.append(copy)

    pass_on(0, wg_ref, full.at[c, x])
    full[c, x] = wg_ref[...]

    zsum = RingSum(lambda r, h: z_chunk.at[r, h], z_got, z_s, z_r, z_ahead, z_behind)

    def settle(k):
        a, bb = sums_y[k].total()
        z_chunk[order[k], 0] = a.astype(BF)
        z_chunk[order[k], 1] = bb.astype(BF)

    def merge(k):
        sums_y[k].merge_a()
        sums_y[k].merge_b()

    merge(0)
    merge(1)
    settle(0)
    zsum.opp_a.start()
    zsum.opp_b.start()
    merge(2)
    settle(1)
    zsum.next_b.start()
    wx.forward()
    for i, o in ((1, 3), (2, 1)):
        slot = full.at[c, lax.rem(x + o, 4)]
        pass_on(i, slot, slot)
    merge(3)
    settle(2)
    zsum.prev_a.start()
    zsum.merge_a()
    zsum.merge_b()
    settle(3)
    wx.finish()
    slot = full.at[c, lax.rem(x + 2, 4)]
    pass_on(3, slot, slot)

    for copy in to_mate:
        copy.wait_recv()

    def rows_of(bb, start, count):
        parts = []
        for _, piece, row, take in packed_rows(start, count):
            parts.append(full[piece % 2, piece // 2, bb, row : row + take, :])
        return parts

    def lay(dst, at, parts, lanes):
        for part in parts:
            dst[at : at + part.shape[0], :] = part[:, lanes]
            at += part.shape[0]

    whole = slice(0, 896)
    for bb in range(NB):
        lay(w_qk, 56 * bb, rows_of(bb, QK_AT, 56), whole)
        for dst, start in ((w_v, V_AT), (w_cq, CQ_AT)):
            parts = rows_of(bb, start, 28)
            lay(dst, 56 * bb, parts, slice(0, 448))
            lay(dst, 56 * bb + 28, parts, slice(448, 896))
        lay(w_so, 28 * bb, rows_of(bb, SO_AT, 28), whole)
        lay(w_co, 28 * bb, rows_of(bb, CO_AT, 28), whole)

    a, bb = zsum.total()
    sums[0:64] = a
    sums[64:128] = bb
    for i in range(NV):
        back_out[i] = sums[4 * i : 4 * i + 4, :].astype(BF)

    def give(o, _):
        to = lax.rem(v + o, NV)
        send(back_out.at[to], back_in.at[v], back_s.at[o], back_r.at[o], (to, b)).start()
        return 0

    lax.fori_loop(1, NV, give, 0)
    back_in[v] = back_out[v]

    def given(o, _):
        send(back_out.at[v], back_in.at[v], back_s.at[o], back_r.at[o], (v, b)).wait_recv()
        return 0

    lax.fori_loop(1, NV, given, 0)
    for i in range(NV):
        back_rows[4 * i : 4 * i + 4, :] = back_in[i].astype(F32)
    start = jnp.dot(sel_ref[...], back_rows[...].astype(BF), preferred_element_type=F32)
    stream = start.astype(BF).astype(F32)

    self_in = normed(stream, ns_ref[...])
    qk = jnp.dot(self_in, w_qk[...], preferred_element_type=F32).astype(BF)
    vals = jnp.dot(self_in, w_v[...], preferred_element_type=F32).astype(BF)
    heads = attend(qk[:, 0:448], qk[:, 448:896], vals)
    stream = stream + jnp.dot(heads, w_so[...], preferred_element_type=F32)
    cross_in = normed(stream, nc_ref[...])
    cross_q = jnp.dot(cross_in, w_cq[...], preferred_element_type=F32).astype(BF)
    spans.wait_recv()
    span_kv = (span_ref[...].astype(F32) + mate_span[...].astype(F32)).astype(BF)
    heads = attend(cross_q, span_kv[:, 0:448], span_kv[:, 448:896])
    stream = stream + jnp.dot(heads, w_co[...], preferred_element_type=F32)
    out_ref[...] = stream.astype(BF)

    def gone(o, _):
        send(back_out.at[v], back_in.at[v], back_s.at[o], back_r.at[o], (v, b)).wait_send()
        return 0

    lax.fori_loop(1, NV, gone, 0)
    for ring in sums_y:
        ring.drain()
    zsum.drain()
    wx.drain()
    for copy in to_mate:
        copy.wait_send()
    spans.wait_send()


def vmem(n):
    return [pl.BlockSpec(memory_space=pltpu.VMEM)] * n


DMA = pltpu.SemaphoreType.DMA


def body(
    neighbour_ids, query_states, table, in_proj, kv_proj, norm_self, self_qkv, self_out,
    norm_cross, cross_q, cross_out,
):
    me = lax.axis_index("vocab")
    table_rows = table.shape[0]
    ids = neighbour_ids.reshape(-1)
    owner = ids // table_rows
    earlier = jnp.arange(128)[:, None] > jnp.arange(128)[None, :]
    within = jnp.sum((owner[:, None] == owner[None, :]) & earlier, axis=1, dtype=jnp.int32)
    slot = owner * 4 + within
    lanes = jnp.arange(128, dtype=jnp.int32)
    selector = (slot[:, None] == lanes[None, :]).astype(BF)
    mine = (owner[:, None] == jnp.arange(NV, dtype=jnp.int32)[None, :])[:, :, None]
    here = ((4 * me + within)[:, None] == lanes[None, :])[:, None, :]
    asks = jnp.sum(jnp.where(mine & here, ids[:, None, None] + 1, 0), axis=0)

    wanted, span, wg = pl.pallas_call(
        first_kernel,
        out_shape=[
            jax.ShapeDtypeStruct((NB, 128), jnp.int32),
            jax.ShapeDtypeStruct((64, 896), BF),
            jax.ShapeDtypeStruct((NB, PIECE, 896), BF),
        ],
        in_specs=vmem(7),
        out_specs=vmem(3),
        scratch_shapes=[
            pltpu.VMEM((NV, 1, 128), jnp.int32),
            pltpu.VMEM((1, 128), jnp.int32),
            pltpu.VMEM((NB, 1, 128), jnp.int32),
            pltpu.VMEM((8, PIECE, 896), BF),
            pltpu.VMEM((4, 4, PIECE, 896), BF),
            pltpu.VMEM((4, 2, 64, 896), BF),
            pltpu.VMEM((6, 64, 896), BF),
            pltpu.VMEM((2, 64, 896), BF),
            pltpu.VMEM((64, 896), BF),
            DMA((NV,)), DMA((NV,)), DMA((NB,)), DMA((NB,)), DMA((3,)), DMA((3,)),
            DMA((4,)), DMA((4,)), DMA((6,)), DMA((6,)), DMA, DMA,
        ],
        compiler_params=pltpu.CompilerParams(
            collective_id=0, has_side_effects=True, vmem_limit_bytes=VMEM_LIMIT
        ),
        name="first",
    )(asks.reshape(NV, 1, 128), query_states.reshape(4, 128, 256), kv_proj, self_qkv, self_out, cross_q, cross_out)

    rows = jnp.clip(wanted - 1 - me * table_rows, 0, table_rows - 1)
    looked = jnp.take(table, rows, axis=0)

    out = pl.pallas_call(
        second_kernel,
        out_shape=jax.ShapeDtypeStruct((128, 896), BF),
        in_specs=vmem(7),
        out_specs=vmem(1)[0],
        scratch_shapes=[
            pltpu.VMEM((4, 4, 2, 64, 896), BF),
            pltpu.VMEM((4, 6, 64, 896), BF),
            pltpu.VMEM((4, 2, 64, 896), BF),
            pltpu.VMEM((6, 64, 896), BF),
            pltpu.VMEM((128, 896), F32),
            pltpu.VMEM((NV, 4, 896), BF),
            pltpu.VMEM((NV, 4, 896), BF),
            pltpu.VMEM((128, 896), F32),
            pltpu.VMEM((2, 4, NB, PIECE, 896), BF),
            pltpu.VMEM((64, 896), BF),
            pltpu.VMEM((896, 896), BF),
            pltpu.VMEM((896, 448), BF),
            pltpu.VMEM((896, 448), BF),
            pltpu.VMEM((448, 896), BF),
            pltpu.VMEM((448, 896), BF),
            DMA((4, 6)), DMA((4, 6)), DMA((6,)), DMA((6,)), DMA((NV,)), DMA((NV,)),
            DMA((4,)), DMA((4,)), DMA((4,)), DMA((4,)), DMA, DMA,
        ],
        compiler_params=pltpu.CompilerParams(
            collective_id=1, has_side_effects=True, vmem_limit_bytes=VMEM_LIMIT
        ),
        name="second",
    )(looked, in_proj, selector, span, wg, norm_self.reshape(1, 896), norm_cross.reshape(1, 896))
    return out.reshape(1, 128, 896)


def solution(mesh):
    both = ("vocab", "batch")
    in_specs = (
        P(both, None), P("vocab", None, "batch"), P("vocab", "batch"), P("batch", None),
        P("batch", None), P(), P("batch", None), P("batch", None), P(), P("batch", None),
        P("batch", None),
    )
    return jax.shard_map(
        body, mesh=mesh, in_specs=in_specs, out_specs=P(both, None, None), check_vma=False
    )
```

```python
import functools

import jax
import jax.numpy as jnp
from jax import lax
from jax.experimental import pallas as pl
from jax.experimental.pallas import tpu as pltpu
from jax.sharding import PartitionSpec as P

MESH = pl.DeviceIdType.MESH
BF = jnp.bfloat16
F32 = jnp.float32
HEAD = 64
NV = 32
NB = 16
QK_AT, V_AT, CQ_AT, SO_AT, CO_AT = 0, 56, 84, 112, 140
PIECE = 24
VMEM_LIMIT = 60 * 1024 * 1024


def where_am_i():
    v = lax.axis_index("vocab")
    b = lax.axis_index("batch")
    return v, b, v // 8, lax.rem(v, 2), b // 4, lax.rem(b, 4)


def send(src, dst, ssem, rsem, dev):
    return pltpu.make_async_remote_copy(
        src_ref=src, dst_ref=dst, send_sem=ssem, recv_sem=rsem,
        device_id=dev, device_id_type=MESH,
    )


def greet(v, b):
    barrier = pltpu.get_barrier_semaphore()

    def hello_vocab(o, _):
        pl.semaphore_signal(
            barrier, inc=1, device_id=(lax.rem(v + o, NV), b), device_id_type=MESH
        )
        return 0

    lax.fori_loop(1, NV, hello_vocab, 0)

    def hello_batch(o, _):
        pl.semaphore_signal(
            barrier, inc=1, device_id=(v, lax.rem(b + o, NB)), device_id_type=MESH
        )
        return 0

    lax.fori_loop(1, NB, hello_batch, 0)


def all_here():
    pl.semaphore_wait(pltpu.get_barrier_semaphore(), NV - 1 + NB - 1)


class RingSum:
    def __init__(self, chunk, got, ssem, rsem, ahead, behind):
        def m(i, src, dev):
            return send(src, got.at[i], ssem.at[i], rsem.at[i], dev)

        self.chunk, self.got = chunk, got
        self.opp_a = m(0, chunk(2, 0), ahead)
        self.opp_b = m(1, chunk(2, 1), behind)
        self.next_b = m(2, chunk(1, 1), ahead)
        self.prev_a = m(3, chunk(3, 0), behind)
        self.merged_a = m(4, chunk(1, 0), ahead)
        self.merged_b = m(5, chunk(3, 1), behind)

    def merge_a(self):
        self.opp_a.wait_recv()
        ref = self.chunk(1, 0)
        ref[...] = (ref[...].astype(F32) + self.got[0].astype(F32)).astype(BF)
        self.merged_a.start()

    def merge_b(self):
        self.opp_b.wait_recv()
        ref = self.chunk(3, 1)
        ref[...] = (ref[...].astype(F32) + self.got[1].astype(F32)).astype(BF)
        self.merged_b.start()

    def total(self):
        self.prev_a.wait_recv()
        self.merged_a.wait_recv()
        a = self.chunk(0, 0)[...].astype(F32) + self.got[3].astype(F32) + self.got[4].astype(F32)
        self.next_b.wait_recv()
        self.merged_b.wait_recv()
        b = self.chunk(0, 1)[...].astype(F32) + self.got[2].astype(F32) + self.got[5].astype(F32)
        return a, b

    def drain(self):
        for c in (self.opp_a, self.opp_b, self.next_b, self.prev_a, self.merged_a, self.merged_b):
            c.wait_send()


class RingCopies:
    def __init__(self, own, slot, half, me, ssem, rsem, ahead, behind):
        left, right = lax.rem(me + 3, 4), lax.rem(me + 1, 4)
        far = lax.rem(me + 2, 4)
        self.to_ahead = send(own, slot(me), ssem.at[0], rsem.at[0], ahead)
        self.to_behind = send(own, slot(me), ssem.at[1], rsem.at[1], behind)
        self.on_ahead = send(half(left, 0), half(left, 0), ssem.at[2], rsem.at[2], ahead)
        self.on_behind = send(half(right, 1), half(right, 1), ssem.at[3], rsem.at[3], behind)
        self.from_left = (slot(left), rsem.at[0])
        self.from_right = (slot(right), rsem.at[1])
        self.far_a = (half(far, 0), rsem.at[2])
        self.far_b = (half(far, 1), rsem.at[3])

    def start(self):
        self.to_ahead.start()
        self.to_behind.start()

    def forward(self):
        self.to_ahead.wait_recv()
        self.on_ahead.start()
        self.to_behind.wait_recv()
        self.on_behind.start()

    def finish(self):
        self.on_ahead.wait_recv()
        self.on_behind.wait_recv()

    def drain(self):
        for c in (self.to_ahead, self.to_behind, self.on_ahead, self.on_behind):
            c.wait_send()


def packed_rows(start, count):
    done = 0
    while done < count:
        at = start + done
        take = min(count - done, PIECE - at % PIECE)
        yield done, at // PIECE, at % PIECE, take
        done += take


def normed(values, gain):
    scale = lax.rsqrt(jnp.mean(values * values, axis=-1, keepdims=True) + 1e-06)
    return (values * scale * gain).astype(BF)


def softmax(scores):
    e = jnp.exp(scores - jnp.max(scores, axis=-1, keepdims=True))
    return (e / jnp.sum(e, axis=-1, keepdims=True)).astype(BF)


def attend(queries, keys, values):
    outs = []
    for h in range(queries.shape[1] // HEAD):
        cut = slice(h * HEAD, (h + 1) * HEAD)
        scores = lax.dot_general(
            queries[:, cut], keys[:, cut], (((1,), (1,)), ((), ())), preferred_element_type=F32
        ) * HEAD ** (-0.5)
        outs.append(jnp.dot(softmax(scores), values[:, cut], preferred_element_type=F32).astype(BF))
    return jnp.concatenate(outs, axis=1)


TABLE_ROWS = 4000
STEP = 160
ORDER = (2, 1, 3, 0)


def owner_of(ids):
    return jnp.floor((ids.astype(F32) + 0.5) * (1.0 / TABLE_ROWS)).astype(jnp.int32)


def iota(shape, dim):
    return lax.broadcasted_iota(jnp.int32, shape, dim)


def kernel(
    ids_ref, q_ref, kvp_ref, qkv_ref, so_ref, cq_ref, co_ref, inp_ref, ns_ref, nc_ref, table_ref,
    out_ref,
    asks, ids_got, row_ref, rows_got, place, place_smem, table_bf, table_f32, rows_f32, selector,
    pack, wg, full, kv_chunk, kv_got, kv_y, kv_in, span, mate_span,
    chunk, y_got, z_chunk, z_got, sums, back_out, back_in, back_rows,
    w_qk, w_v, w_cq, w_so, w_co,
    local, ids_s, ids_r, row_s, row_r, wz_s, wz_r, wy_s, wy_r, wx_s, wx_r, wc_s, wc_r,
    ky_s, ky_r, kz_s, kz_r, m_s, m_r, y_s, y_r, z_s, z_r, back_s, back_r,
):
    v, b, x, c, y, z = where_am_i()
    greet(v, b)
    rest = lax.rem(v, 8)
    odd = lax.rem(z, 2)
    ahead = (v, lax.rem(y + 1, 4) * 4 + z)
    behind = (v, lax.rem(y + 3, 4) * 4 + z)
    z_ahead = (v, y * 4 + lax.rem(z + 1, 4))
    z_behind = (v, y * 4 + lax.rem(z + 3, 4))
    z_outside = (v, y * 4 + lax.rem(z + 3 + 2 * odd, 4))
    z_mate = (v, y * 4 + z + 1 - 2 * odd)
    x_ahead = (lax.rem(x + 1, 4) * 8 + rest, b)
    x_behind = (lax.rem(x + 3, 4) * 8 + rest, b)
    mate = (v + 1 - 2 * c, b)

    load_table = pltpu.make_async_copy(table_ref, table_bf, local.at[0])
    load_table.start()

    ids_row = jnp.broadcast_to(ids_ref[...], (128, 128))
    ids_col = ids_row.T
    own_row, own_col = owner_of(ids_row), owner_of(ids_col)
    same = own_row == own_col
    up, across = iota((128, 128), 0), iota((128, 128), 1)
    within_col = jnp.sum(jnp.where(same & (across < up), 1.0, 0.0), axis=1, keepdims=True)
    within_row = jnp.sum(jnp.where(same & (up < across), 1.0, 0.0), axis=0, keepdims=True)
    slot = own_col * 4 + within_col.astype(jnp.int32)
    selector[...] = jnp.where(slot == across, 1.0, 0.0).astype(BF)
    mine = iota((NV, 128), 0) == own_row[:NV]
    lane = iota((NV, 128), 1)
    question = jnp.zeros((NV, 128), jnp.int32)
    for j in range(4):
        hit = mine & (within_row == float(j))
        column = jnp.sum(jnp.where(hit, ids_row[:NV] + 1, 0), axis=1, keepdims=True)
        question = jnp.where(lane == 4 * v + j, column, question)
    asks[...] = question.reshape(NV, 1, 128)

    all_here()

    def ask(o, _):
        to = lax.rem(v + o, NV)
        send(asks.at[to], ids_got.at[v], ids_s.at[o], ids_r.at[o], (to, b)).start()
        return 0

    lax.fori_loop(1, NV, ask, 0)

    ky = RingSum(lambda r, h: kv_chunk.at[r, h], kv_got, ky_s, ky_r, ahead, behind)

    def open_ring(ring, r):
        if r == 2:
            ring.opp_a.start()
            ring.opp_b.start()
        elif r == 1:
            ring.next_b.start()
        elif r == 3:
            ring.prev_a.start()

    for r in ORDER:
        term = jnp.dot(q_ref[lax.rem(y + r, 4)], kvp_ref[...], preferred_element_type=F32)
        kv_chunk[r] = term.reshape(2, 64, 896).astype(BF)
        open_ring(ky, r)

    def put(block, start):
        for at, piece, row, take in packed_rows(start, block.shape[0]):
            pack[piece, row : row + take, :] = block[at : at + take]

    put(qkv_ref[:, 0:896], QK_AT)
    put(jnp.concatenate([qkv_ref[0:28, 896:1344], qkv_ref[28:56, 896:1344]], axis=1), V_AT)
    put(jnp.concatenate([cq_ref[0:28, :], cq_ref[28:56, :]], axis=1), CQ_AT)
    put(so_ref[...], SO_AT)
    put(co_ref[...], CO_AT)
    pack[7] = jnp.zeros_like(pack[7])
    wg[y, z] = pack[x * 2 + c]

    load_table.wait()

    def widen(i, _):
        at = pl.ds(pl.multiple_of(i * STEP, STEP), STEP)
        table_f32[at, :] = table_bf[at, :].astype(F32)
        return 0

    lax.fori_loop(0, TABLE_ROWS // STEP, widen, 0)

    def asked(o, _):
        send(asks.at[v], ids_got.at[v], ids_s.at[o], ids_r.at[o], (v, b)).wait_recv()
        return 0

    lax.fori_loop(1, NV, asked, 0)
    ids_got[v] = asks[v]
    row_ref[...] = jnp.sum(ids_got[...], axis=0)

    def tell(o, _):
        to = lax.rem(b + o, NB)
        send(row_ref, rows_got.at[b], row_s.at[o], row_r.at[o], (v, to)).start()
        return 0

    lax.fori_loop(1, NB, tell, 0)
    rows_got[b] = row_ref[...]

    wz = RingCopies(
        wg.at[y, z], lambda i: wg.at[y, i], lambda i, h: wg.at[y, i, pl.ds(8 * h, 8 + 8 * h)],
        z, wz_s, wz_r, z_ahead, z_behind,
    )
    wz.start()
    ky.merge_a()
    ky.merge_b()
    a, bb = ky.total()
    kv_y[0] = a.astype(BF)
    kv_y[1] = bb.astype(BF)
    half_pair = z // 2
    kz = send(kv_y.at[1 - half_pair], kv_in, kz_s, kz_r, z_outside)
    kz.start()
    wz.forward()

    def told(o, _):
        send(row_ref, rows_got.at[b], row_s.at[o], row_r.at[o], (v, b)).wait_recv()
        return 0

    lax.fori_loop(1, NB, told, 0)
    place[...] = jnp.clip(rows_got[:, 0, :] - 1 - v * TABLE_ROWS, 0, TABLE_ROWS - 1)
    to_scalars = pltpu.make_async_copy(place, place_smem, local.at[1])
    to_scalars.start()
    to_scalars.wait()

    rings = [
        RingSum(lambda r, h, k=k: chunk.at[k, r, h], y_got.at[k], y_s.at[k], y_r.at[k], ahead, behind)
        for k in range(4)
    ]

    def project(k, r):
        peer = lax.rem(y + r, 4) * 4 + lax.rem(z + ORDER[k], 4)

        def eight(i, _):
            for u in range(8):
                at = place_smem[peer, i * 8 + u]
                rows_f32[pl.ds(pl.multiple_of(i * 8, 8) + u, 1), :] = table_f32[pl.ds(at, 1), :]
            return 0

        lax.fori_loop(0, 16, eight, 0)
        term = jnp.dot(rows_f32[...].astype(BF), inp_ref[...], preferred_element_type=F32)
        chunk[k, r] = term.reshape(2, 64, 896).astype(BF)

    zsum = RingSum(lambda r, h: z_chunk.at[r, h], z_got, z_s, z_r, z_ahead, z_behind)

    def settle(k):
        a, bb = rings[k].total()
        z_chunk[ORDER[k], 0] = a.astype(BF)
        z_chunk[ORDER[k], 1] = bb.astype(BF)

    def merge(k):
        rings[k].merge_a()
        rings[k].merge_b()

    def go(k, *which):
        for r in which:
            project(k, r)
            open_ring(rings[k], r)

    go(0, 2, 1, 3)
    go(1, 2)
    project(0, 0)
    merge(0)
    go(1, 1, 3)
    go(2, 2)
    merge(1)
    project(1, 0)
    settle(0)
    zsum.opp_a.start()
    zsum.opp_b.start()
    go(2, 1, 3)
    wz.finish()
    wy = RingCopies(
        wg.at[y], lambda i: wg.at[i], lambda i, h: wg.at[i, pl.ds(2 * h, 2)], y, wy_s, wy_r,
        ahead, behind,
    )
    wy.start()
    go(3, 2)
    merge(2)
    project(2, 0)
    settle(1)
    zsum.next_b.start()
    go(3, 1, 3)
    merge(3)
    wy.forward()
    project(3, 0)
    settle(2)
    zsum.prev_a.start()
    zsum.merge_a()
    zsum.merge_b()
    kz.wait_recv()
    span[...] = (kv_y[half_pair].astype(F32) + kv_in[...].astype(F32)).astype(BF)
    spans = send(span, mate_span, m_s, m_r, z_mate)
    spans.start()
    settle(3)
    wy.finish()

    wx = RingCopies(
        wg, lambda i: full.at[c, i], lambda i, h: full.at[c, i, pl.ds(2 * h, 2)], x,
        wx_s, wx_r, x_ahead, x_behind,
    )
    wx.start()
    to_mate = []

    def pass_on(i, src, dst):
        copy = send(src, dst, wc_s.at[i], wc_r.at[i], mate)
        copy.start()
        to_mate.append(copy)

    pass_on(0, wg, full.at[c, x])
    full[c, x] = wg[...]
    wx.forward()
    for i, o in ((1, 3), (2, 1)):
        slot_ref = full.at[c, lax.rem(x + o, 4)]
        pass_on(i, slot_ref, slot_ref)
    wx.finish()
    slot_ref = full.at[c, lax.rem(x + 2, 4)]
    pass_on(3, slot_ref, slot_ref)

    for copy in to_mate:
        copy.wait_recv()

    def rows_of(peer, start, count):
        return [
            full[piece % 2, piece // 2, peer // 4, peer % 4, row : row + take, :]
            for _, piece, row, take in packed_rows(start, count)
        ]

    def lay(dst, at, parts, lanes):
        for part in parts:
            dst[at : at + part.shape[0], :] = part[:, lanes]
            at += part.shape[0]

    whole = slice(0, 896)
    for peer in range(NB):
        lay(w_qk, 56 * peer, rows_of(peer, QK_AT, 56), whole)
        for dst, start in ((w_v, V_AT), (w_cq, CQ_AT)):
            parts = rows_of(peer, start, 28)
            lay(dst, 56 * peer, parts, slice(0, 448))
            lay(dst, 56 * peer + 28, parts, slice(448, 896))
        lay(w_so, 28 * peer, rows_of(peer, SO_AT, 28), whole)
        lay(w_co, 28 * peer, rows_of(peer, CO_AT, 28), whole)

    a, bb = zsum.total()
    sums[0:64] = a
    sums[64:128] = bb
    for i in range(NV):
        back_out[i] = sums[4 * i : 4 * i + 4, :].astype(BF)

    def give(o, _):
        to = lax.rem(v + o, NV)
        send(back_out.at[to], back_in.at[v], back_s.at[o], back_r.at[o], (to, b)).start()
        return 0

    lax.fori_loop(1, NV, give, 0)
    back_in[v] = back_out[v]

    def given(o, _):
        send(back_out.at[v], back_in.at[v], back_s.at[o], back_r.at[o], (v, b)).wait_recv()
        return 0

    lax.fori_loop(1, NV, given, 0)
    for i in range(NV):
        back_rows[4 * i : 4 * i + 4, :] = back_in[i].astype(F32)
    start = jnp.dot(selector[...], back_rows[...].astype(BF), preferred_element_type=F32)
    stream = start.astype(BF).astype(F32)

    self_in = normed(stream, ns_ref[...])
    qk = jnp.dot(self_in, w_qk[...], preferred_element_type=F32).astype(BF)
    vals = jnp.dot(self_in, w_v[...], preferred_element_type=F32).astype(BF)
    heads = attend(qk[:, 0:448], qk[:, 448:896], vals)
    stream = stream + jnp.dot(heads, w_so[...], preferred_element_type=F32)
    cross_in = normed(stream, nc_ref[...])
    cross_q = jnp.dot(cross_in, w_cq[...], preferred_element_type=F32).astype(BF)
    spans.wait_recv()
    span_kv = (span[...].astype(F32) + mate_span[...].astype(F32)).astype(BF)
    heads = attend(cross_q, span_kv[:, 0:448], span_kv[:, 448:896])
    stream = stream + jnp.dot(heads, w_co[...], preferred_element_type=F32)
    out_ref[...] = stream.astype(BF)

    def sent(count, src, dst, ssem, rsem):
        def one(o, _):
            send(src, dst, ssem.at[o], rsem.at[o], (v, b)).wait_send()
            return 0

        lax.fori_loop(1, count, one, 0)

    sent(NV, asks.at[v], ids_got.at[v], ids_s, ids_r)
    sent(NB, row_ref, rows_got.at[b], row_s, row_r)
    sent(NV, back_out.at[v], back_in.at[v], back_s, back_r)
    for ring in (ky, *rings, zsum, wz, wy, wx):
        ring.drain()
    for copy in (*to_mate, kz, spans):
        copy.wait_send()


DMA = pltpu.SemaphoreType.DMA


def body(
    neighbour_ids, query_states, table, in_proj, kv_proj, norm_self, self_qkv, self_out,
    norm_cross, cross_q, cross_out,
):
    vm = pltpu.VMEM
    out = pl.pallas_call(
        kernel,
        out_shape=jax.ShapeDtypeStruct((128, 896), BF),
        in_specs=[pl.BlockSpec(memory_space=vm)] * 10 + [pl.BlockSpec(memory_space=pl.ANY)],
        out_specs=pl.BlockSpec(memory_space=vm),
        scratch_shapes=[
            vm((NV, 1, 128), jnp.int32), vm((NV, 1, 128), jnp.int32), vm((1, 128), jnp.int32),
            vm((NB, 1, 128), jnp.int32), vm((NB, 128), jnp.int32), pltpu.SMEM((NB, 128), jnp.int32),
            vm((TABLE_ROWS, 256), BF), vm((TABLE_ROWS, 256), F32), vm((128, 256), F32),
            vm((128, 128), BF),
            vm((8, PIECE, 896), BF), vm((4, 4, PIECE, 896), BF), vm((2, 4, 4, 4, PIECE, 896), BF),
            vm((4, 2, 64, 896), BF), vm((6, 64, 896), BF), vm((2, 64, 896), BF),
            vm((64, 896), BF), vm((64, 896), BF), vm((64, 896), BF),
            vm((4, 4, 2, 64, 896), BF), vm((4, 6, 64, 896), BF), vm((4, 2, 64, 896), BF),
            vm((6, 64, 896), BF), vm((128, 896), F32), vm((NV, 4, 896), BF), vm((NV, 4, 896), BF),
            vm((128, 896), F32),
            vm((896, 896), BF), vm((896, 448), BF), vm((896, 448), BF), vm((448, 896), BF),
            vm((448, 896), BF),
            DMA((2,)), DMA((NV,)), DMA((NV,)), DMA((NB,)), DMA((NB,)),
            DMA((4,)), DMA((4,)), DMA((4,)), DMA((4,)), DMA((4,)), DMA((4,)), DMA((4,)), DMA((4,)),
            DMA((6,)), DMA((6,)), DMA, DMA, DMA, DMA, DMA((4, 6)), DMA((4, 6)),
            DMA((6,)), DMA((6,)), DMA((NV,)), DMA((NV,)),
        ],
        compiler_params=pltpu.CompilerParams(
            collective_id=0, has_side_effects=True, vmem_limit_bytes=VMEM_LIMIT
        ),
        name="encoder",
    )(
        neighbour_ids, query_states.reshape(4, 128, 256), kv_proj, self_qkv, self_out, cross_q,
        cross_out, in_proj, norm_self.reshape(1, 896), norm_cross.reshape(1, 896), table,
    )
    return out.reshape(1, 128, 896)


def solution(mesh):
    both = ("vocab", "batch")
    in_specs = (
        P(both, None), P("vocab", None, "batch"), P("vocab", "batch"), P("batch", None),
        P("batch", None), P(), P("batch", None), P("batch", None), P(), P("batch", None),
        P("batch", None),
    )
    return jax.shard_map(
        body, mesh=mesh, in_specs=in_specs, out_specs=P(both, None, None), check_vma=False
    )
```

```python
import functools

import jax
import jax.numpy as jnp
from jax import lax
from jax.experimental import pallas as pl
from jax.experimental.pallas import tpu as pltpu
from jax.sharding import PartitionSpec as P

MESH = pl.DeviceIdType.MESH
BF = jnp.bfloat16
F32 = jnp.float32
HEAD = 64
NV = 32
NB = 16
QK_AT, V_AT, CQ_AT, SO_AT, CO_AT = 0, 56, 84, 112, 140
PIECE = 24
VMEM_LIMIT = 60 * 1024 * 1024


def where_am_i():
    v = lax.axis_index("vocab")
    b = lax.axis_index("batch")
    return v, b, v // 8, lax.rem(v, 2), b // 4, lax.rem(b, 4)


def send(src, dst, ssem, rsem, dev):
    return pltpu.make_async_remote_copy(
        src_ref=src, dst_ref=dst, send_sem=ssem, recv_sem=rsem,
        device_id=dev, device_id_type=MESH,
    )


def greet(v, b):
    barrier = pltpu.get_barrier_semaphore()

    def hello_vocab(o, _):
        pl.semaphore_signal(
            barrier, inc=1, device_id=(lax.rem(v + o, NV), b), device_id_type=MESH
        )
        return 0

    lax.fori_loop(1, NV, hello_vocab, 0)

    def hello_batch(o, _):
        pl.semaphore_signal(
            barrier, inc=1, device_id=(v, lax.rem(b + o, NB)), device_id_type=MESH
        )
        return 0

    lax.fori_loop(1, NB, hello_batch, 0)


def all_here():
    pl.semaphore_wait(pltpu.get_barrier_semaphore(), NV - 1 + NB - 1)


class RingSum:
    def __init__(self, chunk, got, ssem, rsem, ahead, behind):
        def m(i, src, dev):
            return send(src, got.at[i], ssem.at[i], rsem.at[i], dev)

        self.chunk, self.got = chunk, got
        self.opp_a = m(0, chunk(2, 0), ahead)
        self.opp_b = m(1, chunk(2, 1), behind)
        self.next_b = m(2, chunk(1, 1), ahead)
        self.prev_a = m(3, chunk(3, 0), behind)
        self.merged_a = m(4, chunk(1, 0), ahead)
        self.merged_b = m(5, chunk(3, 1), behind)

    def merge_a(self):
        self.opp_a.wait_recv()
        ref = self.chunk(1, 0)
        ref[...] = (ref[...].astype(F32) + self.got[0].astype(F32)).astype(BF)
        self.merged_a.start()

    def merge_b(self):
        self.opp_b.wait_recv()
        ref = self.chunk(3, 1)
        ref[...] = (ref[...].astype(F32) + self.got[1].astype(F32)).astype(BF)
        self.merged_b.start()

    def total(self):
        self.prev_a.wait_recv()
        self.merged_a.wait_recv()
        a = self.chunk(0, 0)[...].astype(F32) + self.got[3].astype(F32) + self.got[4].astype(F32)
        self.next_b.wait_recv()
        self.merged_b.wait_recv()
        b = self.chunk(0, 1)[...].astype(F32) + self.got[2].astype(F32) + self.got[5].astype(F32)
        return a, b

    def drain(self):
        for c in (self.opp_a, self.opp_b, self.next_b, self.prev_a, self.merged_a, self.merged_b):
            c.wait_send()


class RingCopies:
    def __init__(self, own, slot, half, me, ssem, rsem, ahead, behind):
        left, right = lax.rem(me + 3, 4), lax.rem(me + 1, 4)
        far = lax.rem(me + 2, 4)
        self.to_ahead = send(own, slot(me), ssem.at[0], rsem.at[0], ahead)
        self.to_behind = send(own, slot(me), ssem.at[1], rsem.at[1], behind)
        self.on_ahead = send(half(left, 0), half(left, 0), ssem.at[2], rsem.at[2], ahead)
        self.on_behind = send(half(right, 1), half(right, 1), ssem.at[3], rsem.at[3], behind)
        self.from_left = (slot(left), rsem.at[0])
        self.from_right = (slot(right), rsem.at[1])
        self.far_a = (half(far, 0), rsem.at[2])
        self.far_b = (half(far, 1), rsem.at[3])

    def start(self):
        self.to_ahead.start()
        self.to_behind.start()

    def forward(self):
        self.to_ahead.wait_recv()
        self.on_ahead.start()
        self.to_behind.wait_recv()
        self.on_behind.start()

    def finish(self):
        self.on_ahead.wait_recv()
        self.on_behind.wait_recv()

    def drain(self):
        for c in (self.to_ahead, self.to_behind, self.on_ahead, self.on_behind):
            c.wait_send()


def packed_rows(start, count):
    done = 0
    while done < count:
        at = start + done
        take = min(count - done, PIECE - at % PIECE)
        yield done, at // PIECE, at % PIECE, take
        done += take


def normed(values, gain):
    scale = lax.rsqrt(jnp.mean(values * values, axis=-1, keepdims=True) + 1e-06)
    return (values * scale * gain).astype(BF)


def softmax(scores):
    e = jnp.exp(scores - jnp.max(scores, axis=-1, keepdims=True))
    return (e / jnp.sum(e, axis=-1, keepdims=True)).astype(BF)


def attend(queries, keys, values):
    outs = []
    for h in range(queries.shape[1] // HEAD):
        cut = slice(h * HEAD, (h + 1) * HEAD)
        scores = lax.dot_general(
            queries[:, cut], keys[:, cut], (((1,), (1,)), ((), ())), preferred_element_type=F32
        ) * HEAD ** (-0.5)
        outs.append(jnp.dot(softmax(scores), values[:, cut], preferred_element_type=F32).astype(BF))
    return jnp.concatenate(outs, axis=1)


TABLE_ROWS = 4000
STEP = 160
ORDER = (2, 1, 3, 0)
GROUPS = ((2, 2), (3, 1), (1, 3), (0, 0))


def owner_of(ids):
    return jnp.floor((ids.astype(F32) + 0.5) * (1.0 / TABLE_ROWS)).astype(jnp.int32)


def iota(shape, dim):
    return lax.broadcasted_iota(jnp.int32, shape, dim)


def kernel(
    ids_ref, ns_ref, nc_ref, q_in, kvp_in, qkv_in, so_in, cq_in, co_in, inp_in, table_ref,
    out_ref,
    q_ref, kvp_ref, qkv_ref, so_ref, cq_ref, co_ref, inp_ref,
    asks, ids_got, row_ref, rows_got, place, place_smem, table_bf, table_f32, rows_f32, selector,
    pack, wg, full, kv_chunk, kv_got, kv_y, kv_in, span, mate_span,
    chunk, y_got, z_chunk, z_got, sums, back_out, back_in, back_rows,
    w_qk, w_v, w_cq, w_so, w_co,
    local, ids_s, ids_r, row_s, row_r, wz_s, wz_r, wy_s, wy_r, wx_s, wx_r, wc_s, wc_r,
    ky_s, ky_r, kz_s, kz_r, m_s, m_r, e_s, e_r, y_s, y_r, z_s, z_r, back_s, back_r,
):
    v, b, x, c, y, z = where_am_i()
    greet(v, b)
    rest = lax.rem(v, 8)
    odd = lax.rem(z, 2)
    ahead = (v, lax.rem(y + 1, 4) * 4 + z)
    behind = (v, lax.rem(y + 3, 4) * 4 + z)
    z_ahead = (v, y * 4 + lax.rem(z + 1, 4))
    z_behind = (v, y * 4 + lax.rem(z + 3, 4))
    z_outside = (v, y * 4 + lax.rem(z + 3 + 2 * odd, 4))
    z_mate = (v, y * 4 + z + 1 - 2 * odd)
    x_ahead = (lax.rem(x + 1, 4) * 8 + rest, b)
    x_behind = (lax.rem(x + 3, 4) * 8 + rest, b)
    mate = (v + 1 - 2 * c, b)

    pairs = (
        (table_ref, table_bf), (None, None), (qkv_in, qkv_ref), (so_in, so_ref), (cq_in, cq_ref),
        (co_in, co_ref), (q_in, q_ref), (kvp_in, kvp_ref), (inp_in, inp_ref),
    )
    loads = [
        pltpu.make_async_copy(src, dst, local.at[i]) if src is not None else None
        for i, (src, dst) in enumerate(pairs)
    ]
    for i in (2, 3, 4, 5, 6, 7, 0, 8):
        loads[i].start()

    ids_row = jnp.broadcast_to(ids_ref[...], (128, 128))
    ids_col = ids_row.T
    own_row, own_col = owner_of(ids_row), owner_of(ids_col)
    same = own_row == own_col
    up, across = iota((128, 128), 0), iota((128, 128), 1)
    within_col = jnp.sum(jnp.where(same & (across < up), 1.0, 0.0), axis=1, keepdims=True)
    within_row = jnp.sum(jnp.where(same & (up < across), 1.0, 0.0), axis=0, keepdims=True)
    slot = own_col * 4 + within_col.astype(jnp.int32)
    selector[...] = jnp.where(slot == across, 1.0, 0.0).astype(BF)
    mine = iota((NV, 128), 0) == own_row[:NV]
    lane = iota((NV, 128), 1)
    question = jnp.zeros((NV, 128), jnp.int32)
    for j in range(4):
        hit = mine & (within_row == float(j))
        column = jnp.sum(jnp.where(hit, ids_row[:NV] + 1, 0), axis=1, keepdims=True)
        question = jnp.where(lane == 4 * v + j, column, question)
    asks[...] = question.reshape(NV, 1, 128)

    all_here()

    def ask(o, _):
        to = lax.rem(v + o, NV)
        send(asks.at[to], ids_got.at[v], ids_s.at[o], ids_r.at[o], (to, b)).start()
        return 0

    lax.fori_loop(1, NV, ask, 0)

    for i in (2, 3, 4, 5):
        loads[i].wait()

    def put(block, start):
        for at, piece, row, take in packed_rows(start, block.shape[0]):
            pack[piece, row : row + take, :] = block[at : at + take]

    put(qkv_ref[:, 0:896], QK_AT)
    put(jnp.concatenate([qkv_ref[0:28, 896:1344], qkv_ref[28:56, 896:1344]], axis=1), V_AT)
    put(jnp.concatenate([cq_ref[0:28, :], cq_ref[28:56, :]], axis=1), CQ_AT)
    put(so_ref[...], SO_AT)
    put(co_ref[...], CO_AT)
    pack[7] = jnp.zeros_like(pack[7])
    wg[y, z] = pack[x * 2 + c]

    wz = RingCopies(
        wg.at[y, z], lambda i: wg.at[y, i], lambda i, h: wg.at[y, i, pl.ds(8 * h, 8 + 8 * h)],
        z, wz_s, wz_r, z_ahead, z_behind,
    )
    wz.start()

    ky = RingSum(lambda r, h: kv_chunk.at[r, h], kv_got, ky_s, ky_r, ahead, behind)

    def open_ring(ring, r):
        if r == 2:
            ring.opp_a.start()
            ring.opp_b.start()
        elif r == 1:
            ring.next_b.start()
        elif r == 3:
            ring.prev_a.start()

    loads[6].wait()
    loads[7].wait()
    for r in ORDER:
        term = jnp.dot(q_ref[lax.rem(y + r, 4)], kvp_ref[...], preferred_element_type=F32)
        kv_chunk[r] = term.reshape(2, 64, 896).astype(BF)
        open_ring(ky, r)

    loads[0].wait()

    def widen(i, _):
        at = pl.ds(pl.multiple_of(i * STEP, STEP), STEP)
        table_f32[at, :] = table_bf[at, :].astype(F32)
        return 0

    lax.fori_loop(0, TABLE_ROWS // STEP, widen, 0)

    def asked(o, _):
        send(asks.at[v], ids_got.at[v], ids_s.at[o], ids_r.at[o], (v, b)).wait_recv()
        return 0

    lax.fori_loop(1, NV, asked, 0)
    ids_got[v] = asks[v]
    row_ref[...] = jnp.sum(ids_got[...], axis=0)

    def tell(o, _):
        to = lax.rem(b + o, NB)
        send(row_ref, rows_got.at[b], row_s.at[o], row_r.at[o], (v, to)).start()
        return 0

    lax.fori_loop(1, NB, tell, 0)
    rows_got[b] = row_ref[...]

    ky.merge_a()
    ky.merge_b()
    wz.forward()
    a, bb = ky.total()
    kv_y[0] = a.astype(BF)
    kv_y[1] = bb.astype(BF)
    half_pair = z // 2
    part = [pl.ds(0, 32), pl.ds(32, 32)]
    kz = [
        send(kv_y.at[1 - half_pair, part[i]], kv_in.at[part[i]], kz_s.at[i], kz_r.at[i], z_outside)
        for i in range(2)
    ]
    kz[0].start()
    kz[1].start()
    spans = [
        send(span.at[part[i]], mate_span.at[part[i]], m_s.at[i], m_r.at[i], z_mate)
        for i in range(2)
    ]

    def share_span(i):
        kz[i].wait_recv()
        total = kv_y[half_pair, part[i]].astype(F32) + kv_in[part[i]].astype(F32)
        span[part[i]] = total.astype(BF)
        spans[i].start()

    wz.finish()
    wy = RingCopies(
        wg.at[y], lambda i: wg.at[i], lambda i, h: wg.at[i, pl.ds(2 * h, 2)], y, wy_s, wy_r,
        ahead, behind,
    )
    wy.start()

    def told(o, _):
        send(row_ref, rows_got.at[b], row_s.at[o], row_r.at[o], (v, b)).wait_recv()
        return 0

    lax.fori_loop(1, NB, told, 0)
    place[...] = jnp.clip(rows_got[:, 0, :] - 1 - v * TABLE_ROWS, 0, TABLE_ROWS - 1)
    to_scalars = pltpu.make_async_copy(place, place_smem, local.at[1])
    to_scalars.start()
    to_scalars.wait()
    loads[8].wait()

    rings = [
        RingSum(lambda r, h, k=k: chunk.at[k, r, h], y_got.at[k], y_s.at[k], y_r.at[k], ahead, behind)
        for k in range(1, 4)
    ]
    early = [
        RingSum(
            lambda r, h, i=i: chunk.at[0, r, h, part[i]], y_got.at[0, :, part[i]], e_s.at[i],
            e_r.at[i], ahead, behind,
        )
        for i in range(2)
    ]

    def project(k, r):
        for h in range(2):
            peer = lax.rem(y + r, 4) * 4 + lax.rem(z + GROUPS[k][h], 4)

            def eight(i, _, h=h, peer=peer):
                for u in range(8):
                    at = place_smem[peer, 64 * h + i * 8 + u]
                    to = pl.ds(pl.multiple_of(i * 8, 8) + 64 * h + u, 1)
                    rows_f32[to, :] = table_f32[pl.ds(at, 1), :]
                return 0

            lax.fori_loop(0, 8, eight, 0)
        term = jnp.dot(rows_f32[...].astype(BF), inp_ref[...], preferred_element_type=F32)
        chunk[k, r] = term.reshape(2, 64, 896).astype(BF)

    zsum = [
        RingSum(
            lambda r, h, i=i: z_chunk.at[r, h, part[i]], z_got.at[:, part[i]], z_s.at[i],
            z_r.at[i], z_ahead, z_behind,
        )
        for i in range(2)
    ]

    def settle_early(i):
        a, bb = early[i].total()
        z_chunk[2, 0, part[i]] = a.astype(BF)
        z_chunk[2, 1, part[i]] = bb.astype(BF)
        zsum[i].opp_a.start()
        zsum[i].opp_b.start()

    def settle(k):
        a, bb = rings[k - 1].total()
        z_chunk[GROUPS[k][0], 0] = a.astype(BF)
        z_chunk[GROUPS[k][1], 1] = bb.astype(BF)

    def merge(k):
        rings[k - 1].merge_a()
        rings[k - 1].merge_b()

    def go(k, *which):
        for r in which:
            project(k, r)
            open_ring(rings[k - 1], r)

    to_mate = []

    def pass_on(i, src, dst):
        copy = send(src, dst, wc_s.at[i], wc_r.at[i], mate)
        copy.start()
        to_mate.append(copy)

    project(0, 2)
    open_ring(early[0], 2)
    project(0, 1)
    open_ring(early[0], 1)
    share_span(0)
    open_ring(early[1], 2)
    project(0, 3)
    open_ring(early[0], 3)
    early[0].merge_a()
    early[0].merge_b()
    open_ring(early[1], 1)
    open_ring(early[1], 3)
    project(0, 0)
    early[1].merge_a()
    early[1].merge_b()
    go(1, 2)
    settle_early(0)
    wy.forward()
    go(1, 1)
    settle_early(1)
    go(1, 3)
    share_span(1)

    wy.finish()
    wx = RingCopies(
        wg, lambda i: full.at[c, i], lambda i, h: full.at[c, i, pl.ds(2 * h, 2)], x,
        wx_s, wx_r, x_ahead, x_behind,
    )
    wx.start()
    pass_on(0, wg, full.at[c, x])

    project(2, 2)
    merge(1)
    open_ring(rings[1], 2)
    go(2, 1, 3)
    project(1, 0)
    settle(1)
    for i in range(2):
        zsum[i].next_b.start()
        zsum[i].prev_a.start()
    full[c, x] = wg[...]
    project(3, 2)
    merge(2)
    open_ring(rings[2], 2)
    go(3, 1, 3)
    project(2, 0)
    settle(2)
    project(3, 0)
    zsum[0].merge_a()
    zsum[0].merge_b()
    merge(3)
    zsum[1].merge_a()
    zsum[1].merge_b()
    wx.forward()
    for i, o in ((1, 3), (2, 1)):
        slot_ref = full.at[c, lax.rem(x + o, 4)]
        pass_on(i, slot_ref, slot_ref)
    settle(3)
    wx.finish()
    slot_ref = full.at[c, lax.rem(x + 2, 4)]
    pass_on(3, slot_ref, slot_ref)

    for i in range(2):
        a, bb = zsum[i].total()
        sums[0:32] = a
        sums[32:64] = bb
        for h in range(2):
            for q in range(8):
                row = 32 * h + 4 * q
                back_out[16 * h + 8 * i + q] = sums[row : row + 4, :].astype(BF)

        def give(n, _, i=i):
            to = n + 8 * (n // 8) + 8 * i
            o = lax.rem(to - v + NV, NV)

            @pl.when(o != 0)
            def _():
                send(back_out.at[to], back_in.at[v], back_s.at[o], back_r.at[o], (to, b)).start()

            return 0

        lax.fori_loop(0, 16, give, 0)
    back_in[v] = back_out[v]

    for copy in to_mate:
        copy.wait_recv()

    def rows_of(peer, start, count):
        return [
            full[piece % 2, piece // 2, peer // 4, peer % 4, row : row + take, :]
            for _, piece, row, take in packed_rows(start, count)
        ]

    def lay(dst, at, parts, lanes):
        for part in parts:
            dst[at : at + part.shape[0], :] = part[:, lanes]
            at += part.shape[0]

    whole = slice(0, 896)
    for peer in range(NB):
        lay(w_qk, 56 * peer, rows_of(peer, QK_AT, 56), whole)
        for dst, start in ((w_v, V_AT), (w_cq, CQ_AT)):
            parts = rows_of(peer, start, 28)
            lay(dst, 56 * peer, parts, slice(0, 448))
            lay(dst, 56 * peer + 28, parts, slice(448, 896))
        lay(w_so, 28 * peer, rows_of(peer, SO_AT, 28), whole)
        lay(w_co, 28 * peer, rows_of(peer, CO_AT, 28), whole)

    def given(o, _):
        send(back_out.at[v], back_in.at[v], back_s.at[o], back_r.at[o], (v, b)).wait_recv()
        return 0

    lax.fori_loop(1, NV, given, 0)
    for i in range(NV):
        back_rows[4 * i : 4 * i + 4, :] = back_in[i].astype(F32)
    start = jnp.dot(selector[...], back_rows[...].astype(BF), preferred_element_type=F32)
    stream = start.astype(BF).astype(F32)

    self_in = normed(stream, ns_ref[...].reshape(1, 896))
    qk = jnp.dot(self_in, w_qk[...], preferred_element_type=F32).astype(BF)
    vals = jnp.dot(self_in, w_v[...], preferred_element_type=F32).astype(BF)
    heads = attend(qk[:, 0:448], qk[:, 448:896], vals)
    stream = stream + jnp.dot(heads, w_so[...], preferred_element_type=F32)
    cross_in = normed(stream, nc_ref[...].reshape(1, 896))
    cross_q = jnp.dot(cross_in, w_cq[...], preferred_element_type=F32).astype(BF)
    spans[0].wait_recv()
    spans[1].wait_recv()
    span_kv = (span[...].astype(F32) + mate_span[...].astype(F32)).astype(BF)
    heads = attend(cross_q, span_kv[:, 0:448], span_kv[:, 448:896])
    stream = stream + jnp.dot(heads, w_co[...], preferred_element_type=F32)
    out_ref[...] = stream.astype(BF)

    def sent(count, src, dst, ssem, rsem):
        def one(o, _):
            send(src, dst, ssem.at[o], rsem.at[o], (v, b)).wait_send()
            return 0

        lax.fori_loop(1, count, one, 0)

    sent(NV, asks.at[v], ids_got.at[v], ids_s, ids_r)
    sent(NB, row_ref, rows_got.at[b], row_s, row_r)
    sent(NV, back_out.at[v], back_in.at[v], back_s, back_r)
    for ring in (ky, *early, *rings, *zsum, wz, wy, wx):
        ring.drain()
    for copy in (*to_mate, *kz, *spans):
        copy.wait_send()


DMA = pltpu.SemaphoreType.DMA


def body(
    neighbour_ids, query_states, table, in_proj, kv_proj, norm_self, self_qkv, self_out,
    norm_cross, cross_q, cross_out,
):
    vm = pltpu.VMEM
    out = pl.pallas_call(
        kernel,
        out_shape=jax.ShapeDtypeStruct((128, 896), BF),
        in_specs=[pl.BlockSpec(memory_space=vm)] * 3 + [pl.BlockSpec(memory_space=pl.ANY)] * 8,
        out_specs=pl.BlockSpec(memory_space=vm),
        scratch_shapes=[
            vm((4, 128, 256), BF), vm((256, 896), BF), vm((56, 1344), BF), vm((28, 896), BF),
            vm((56, 448), BF), vm((28, 896), BF), vm((256, 896), BF),
            vm((NV, 1, 128), jnp.int32), vm((NV, 1, 128), jnp.int32), vm((1, 128), jnp.int32),
            vm((NB, 1, 128), jnp.int32), vm((NB, 128), jnp.int32), pltpu.SMEM((NB, 128), jnp.int32),
            vm((TABLE_ROWS, 256), BF), vm((TABLE_ROWS, 256), F32), vm((128, 256), F32),
            vm((128, 128), BF),
            vm((8, PIECE, 896), BF), vm((4, 4, PIECE, 896), BF), vm((2, 4, 4, 4, PIECE, 896), BF),
            vm((4, 2, 64, 896), BF), vm((6, 64, 896), BF), vm((2, 64, 896), BF),
            vm((64, 896), BF), vm((64, 896), BF), vm((64, 896), BF),
            vm((4, 4, 2, 64, 896), BF), vm((4, 6, 64, 896), BF), vm((4, 2, 64, 896), BF),
            vm((6, 64, 896), BF), vm((64, 896), F32), vm((NV, 4, 896), BF), vm((NV, 4, 896), BF),
            vm((128, 896), F32),
            vm((896, 896), BF), vm((896, 448), BF), vm((896, 448), BF), vm((448, 896), BF),
            vm((448, 896), BF),
            DMA((9,)), DMA((NV,)), DMA((NV,)), DMA((NB,)), DMA((NB,)),
            DMA((4,)), DMA((4,)), DMA((4,)), DMA((4,)), DMA((4,)), DMA((4,)), DMA((4,)), DMA((4,)),
            DMA((6,)), DMA((6,)), DMA((2,)), DMA((2,)), DMA((2,)), DMA((2,)),
            DMA((2, 6)), DMA((2, 6)), DMA((4, 6)), DMA((4, 6)), DMA((2, 6)), DMA((2, 6)),
            DMA((NV,)), DMA((NV,)),
        ],
        compiler_params=pltpu.CompilerParams(
            collective_id=0, has_side_effects=True, vmem_limit_bytes=VMEM_LIMIT
        ),
        name="encoder",
    )(
        neighbour_ids, norm_self, norm_cross, query_states.reshape(4, 128, 256), kv_proj, self_qkv,
        self_out, cross_q, cross_out, in_proj, table,
    )
    return out.reshape(1, 128, 896)


def solution(mesh):
    both = ("vocab", "batch")
    in_specs = (
        P(both, None), P("vocab", None, "batch"), P("vocab", "batch"), P("batch", None),
        P("batch", None), P(), P("batch", None), P("batch", None), P(), P("batch", None),
        P("batch", None),
    )
    return jax.shard_map(
        body, mesh=mesh, in_specs=in_specs, out_specs=P(both, None, None), check_vma=False
    )
```

```python
import functools

import jax
import jax.numpy as jnp
from jax import lax
from jax.experimental import pallas as pl
from jax.experimental.pallas import tpu as pltpu
from jax.sharding import PartitionSpec as P

MESH = pl.DeviceIdType.MESH
BF = jnp.bfloat16
F32 = jnp.float32
HEAD = 64
NV = 32
NB = 16
QK_AT, V_AT, CQ_AT, SO_AT, CO_AT = 0, 56, 84, 112, 140
PIECE = 24
VMEM_LIMIT = 60 * 1024 * 1024


def where_am_i():
    v = lax.axis_index("vocab")
    b = lax.axis_index("batch")
    return v, b, v // 8, lax.rem(v, 2), b // 4, lax.rem(b, 4)


def send(src, dst, ssem, rsem, dev):
    return pltpu.make_async_remote_copy(
        src_ref=src, dst_ref=dst, send_sem=ssem, recv_sem=rsem,
        device_id=dev, device_id_type=MESH,
    )


def greet(v, b):
    barrier = pltpu.get_barrier_semaphore()

    def hello_vocab(o, _):
        pl.semaphore_signal(
            barrier, inc=1, device_id=(lax.rem(v + o, NV), b), device_id_type=MESH
        )
        return 0

    lax.fori_loop(1, NV, hello_vocab, 0)

    def hello_batch(o, _):
        pl.semaphore_signal(
            barrier, inc=1, device_id=(v, lax.rem(b + o, NB)), device_id_type=MESH
        )
        return 0

    lax.fori_loop(1, NB, hello_batch, 0)


def all_here():
    pl.semaphore_wait(pltpu.get_barrier_semaphore(), NV - 1 + NB - 1)


class RingSum:
    def __init__(self, chunk, got, ssem, rsem, ahead, behind):
        def m(i, src, dev):
            return send(src, got.at[i], ssem.at[i], rsem.at[i], dev)

        self.chunk, self.got = chunk, got
        self.opp_a = m(0, chunk(2, 0), ahead)
        self.opp_b = m(1, chunk(2, 1), behind)
        self.next_b = m(2, chunk(1, 1), ahead)
        self.prev_a = m(3, chunk(3, 0), behind)
        self.merged_a = m(4, chunk(1, 0), ahead)
        self.merged_b = m(5, chunk(3, 1), behind)

    def merge_a(self):
        self.opp_a.wait_recv()
        ref = self.chunk(1, 0)
        ref[...] = (ref[...].astype(F32) + self.got[0].astype(F32)).astype(BF)
        self.merged_a.start()

    def merge_b(self):
        self.opp_b.wait_recv()
        ref = self.chunk(3, 1)
        ref[...] = (ref[...].astype(F32) + self.got[1].astype(F32)).astype(BF)
        self.merged_b.start()

    def total(self):
        self.prev_a.wait_recv()
        self.merged_a.wait_recv()
        a = self.chunk(0, 0)[...].astype(F32) + self.got[3].astype(F32) + self.got[4].astype(F32)
        self.next_b.wait_recv()
        self.merged_b.wait_recv()
        b = self.chunk(0, 1)[...].astype(F32) + self.got[2].astype(F32) + self.got[5].astype(F32)
        return a, b

    def drain(self):
        for c in (self.opp_a, self.opp_b, self.next_b, self.prev_a, self.merged_a, self.merged_b):
            c.wait_send()


class RingCopies:
    def __init__(self, own, slot, half, me, ssem, rsem, ahead, behind):
        left, right = lax.rem(me + 3, 4), lax.rem(me + 1, 4)
        far = lax.rem(me + 2, 4)
        self.to_ahead = send(own, slot(me), ssem.at[0], rsem.at[0], ahead)
        self.to_behind = send(own, slot(me), ssem.at[1], rsem.at[1], behind)
        self.on_ahead = send(half(left, 0), half(left, 0), ssem.at[2], rsem.at[2], ahead)
        self.on_behind = send(half(right, 1), half(right, 1), ssem.at[3], rsem.at[3], behind)
        self.from_left = (slot(left), rsem.at[0])
        self.from_right = (slot(right), rsem.at[1])
        self.far_a = (half(far, 0), rsem.at[2])
        self.far_b = (half(far, 1), rsem.at[3])

    def start(self):
        self.to_ahead.start()
        self.to_behind.start()

    def forward(self):
        self.to_ahead.wait_recv()
        self.on_ahead.start()
        self.to_behind.wait_recv()
        self.on_behind.start()

    def finish(self):
        self.on_ahead.wait_recv()
        self.on_behind.wait_recv()

    def drain(self):
        for c in (self.to_ahead, self.to_behind, self.on_ahead, self.on_behind):
            c.wait_send()


def packed_rows(start, count):
    done = 0
    while done < count:
        at = start + done
        take = min(count - done, PIECE - at % PIECE)
        yield done, at // PIECE, at % PIECE, take
        done += take


def normed(values, gain):
    scale = lax.rsqrt(jnp.mean(values * values, axis=-1, keepdims=True) + 1e-06)
    return (values * scale * gain).astype(BF)


def softmax(scores):
    e = jnp.exp(scores - jnp.max(scores, axis=-1, keepdims=True))
    return (e / jnp.sum(e, axis=-1, keepdims=True)).astype(BF)


def attend(queries, keys, values):
    outs = []
    for h in range(queries.shape[1] // HEAD):
        cut = slice(h * HEAD, (h + 1) * HEAD)
        scores = lax.dot_general(
            queries[:, cut], keys[:, cut], (((1,), (1,)), ((), ())), preferred_element_type=F32
        ) * HEAD ** (-0.5)
        outs.append(jnp.dot(softmax(scores), values[:, cut], preferred_element_type=F32).astype(BF))
    return jnp.concatenate(outs, axis=1)


TABLE_ROWS = 4000
STEP = 160
ORDER = (2, 1, 3, 0)
GROUPS = ((2, 2), (3, 1), (1, 3), (0, 0))


def owner_of(ids):
    return jnp.floor((ids.astype(F32) + 0.5) * (1.0 / TABLE_ROWS)).astype(jnp.int32)


def iota(shape, dim):
    return lax.broadcasted_iota(jnp.int32, shape, dim)


def kernel(
    ids_ref, ns_ref, nc_ref, q_in, kvp_in, qkv_in, so_in, cq_in, co_in, inp_in, table_ref,
    out_ref,
    q_ref, kvp_ref, qkv_ref, so_ref, cq_ref, co_ref, inp_ref,
    asks, ids_got, row_ref, rows_got, place, place_smem, table_bf, table_f32, rows_f32, selector,
    pack, wg, full, kv_chunk, kv_got, kv_y, kv_in, span, mate_span,
    chunk, y_got, z_chunk, z_got, sums, back_out, back_in, back_rows,
    w_qk, w_v, w_cq, w_so, w_co,
    local, ids_s, ids_r, row_s, row_r, wz_s, wz_r, wy_s, wy_r, wx_s, wx_r, wc_s, wc_r,
    ky_s, ky_r, kz_s, kz_r, m_s, m_r, e_s, e_r, y_s, y_r, z_s, z_r, back_s, back_r,
):
    v, b, x, c, y, z = where_am_i()
    greet(v, b)
    rest = lax.rem(v, 8)
    odd = lax.rem(z, 2)
    ahead = (v, lax.rem(y + 1, 4) * 4 + z)
    behind = (v, lax.rem(y + 3, 4) * 4 + z)
    z_ahead = (v, y * 4 + lax.rem(z + 1, 4))
    z_behind = (v, y * 4 + lax.rem(z + 3, 4))
    z_outside = (v, y * 4 + lax.rem(z + 3 + 2 * odd, 4))
    z_mate = (v, y * 4 + z + 1 - 2 * odd)
    x_ahead = (lax.rem(x + 1, 4) * 8 + rest, b)
    x_behind = (lax.rem(x + 3, 4) * 8 + rest, b)
    mate = (v + 1 - 2 * c, b)

    pairs = (
        (table_ref, table_bf), (None, None), (qkv_in, qkv_ref), (so_in, so_ref), (cq_in, cq_ref),
        (co_in, co_ref), (q_in, q_ref), (kvp_in, kvp_ref), (inp_in, inp_ref),
    )
    loads = [
        pltpu.make_async_copy(src, dst, local.at[i]) if src is not None else None
        for i, (src, dst) in enumerate(pairs)
    ]
    for i in (2, 3, 4, 5, 6, 7, 0, 8):
        loads[i].start()

    ids_row = jnp.broadcast_to(ids_ref[...], (128, 128))
    ids_col = ids_row.T
    own_row, own_col = owner_of(ids_row), owner_of(ids_col)
    same = own_row == own_col
    up, across = iota((128, 128), 0), iota((128, 128), 1)
    within_col = jnp.sum(jnp.where(same & (across < up), 1.0, 0.0), axis=1, keepdims=True)
    within_row = jnp.sum(jnp.where(same & (up < across), 1.0, 0.0), axis=0, keepdims=True)
    slot = own_col * 4 + within_col.astype(jnp.int32)
    selector[...] = jnp.where(slot == across, 1.0, 0.0).astype(BF)
    mine = iota((NV, 128), 0) == own_row[:NV]
    lane = iota((NV, 128), 1)
    question = jnp.zeros((NV, 128), jnp.int32)
    for j in range(4):
        hit = mine & (within_row == float(j))
        column = jnp.sum(jnp.where(hit, ids_row[:NV] + 1, 0), axis=1, keepdims=True)
        question = jnp.where(lane == 4 * v + j, column, question)
    asks[...] = question.reshape(NV, 1, 128)

    all_here()

    def ask(o, _):
        to = lax.rem(v + o, NV)
        send(asks.at[to], ids_got.at[v], ids_s.at[o], ids_r.at[o], (to, b)).start()
        return 0

    lax.fori_loop(1, NV, ask, 0)

    for i in (2, 3, 4, 5):
        loads[i].wait()

    def put(block, start):
        for at, piece, row, take in packed_rows(start, block.shape[0]):
            pack[piece, row : row + take, :] = block[at : at + take]

    put(qkv_ref[:, 0:896], QK_AT)
    put(jnp.concatenate([qkv_ref[0:28, 896:1344], qkv_ref[28:56, 896:1344]], axis=1), V_AT)
    put(jnp.concatenate([cq_ref[0:28, :], cq_ref[28:56, :]], axis=1), CQ_AT)
    put(so_ref[...], SO_AT)
    put(co_ref[...], CO_AT)
    pack[7] = jnp.zeros_like(pack[7])
    wg[y, z] = pack[x * 2 + c]

    wz = RingCopies(
        wg.at[y, z], lambda i: wg.at[y, i], lambda i, h: wg.at[y, i, pl.ds(8 * h, 8 + 8 * h)],
        z, wz_s, wz_r, z_ahead, z_behind,
    )
    wz.start()

    ky = RingSum(lambda r, h: kv_chunk.at[r, h], kv_got, ky_s, ky_r, ahead, behind)

    def open_ring(ring, r):
        if r == 2:
            ring.opp_a.start()
            ring.opp_b.start()
        elif r == 1:
            ring.next_b.start()
        elif r == 3:
            ring.prev_a.start()

    loads[6].wait()
    loads[7].wait()
    for r in ORDER:
        term = jnp.dot(q_ref[lax.rem(y + r, 4)], kvp_ref[...], preferred_element_type=F32)
        kv_chunk[r] = term.reshape(2, 64, 896).astype(BF)
        open_ring(ky, r)

    loads[0].wait()

    def widen(i, _):
        at = pl.ds(pl.multiple_of(i * STEP, STEP), STEP)
        table_f32[at, :] = table_bf[at, :].astype(F32)
        return 0

    lax.fori_loop(0, TABLE_ROWS // STEP, widen, 0)

    def asked(o, _):
        send(asks.at[v], ids_got.at[v], ids_s.at[o], ids_r.at[o], (v, b)).wait_recv()
        return 0

    lax.fori_loop(1, NV, asked, 0)
    ids_got[v] = asks[v]
    row_ref[...] = jnp.sum(ids_got[...], axis=0)

    def tell(o, _):
        to = lax.rem(b + o, NB)
        send(row_ref, rows_got.at[b], row_s.at[o], row_r.at[o], (v, to)).start()
        return 0

    lax.fori_loop(1, NB, tell, 0)
    rows_got[b] = row_ref[...]

    ky.merge_a()
    ky.merge_b()
    wz.forward()
    a, bb = ky.total()
    kv_y[0] = a.astype(BF)
    kv_y[1] = bb.astype(BF)
    half_pair = z // 2
    part = [pl.ds(0, 32), pl.ds(32, 32)]
    kz = [
        send(kv_y.at[1 - half_pair, part[i]], kv_in.at[part[i]], kz_s.at[i], kz_r.at[i], z_outside)
        for i in range(2)
    ]
    kz[0].start()
    kz[1].start()
    spans = [
        send(span.at[part[i]], mate_span.at[part[i]], m_s.at[i], m_r.at[i], z_mate)
        for i in range(2)
    ]

    def share_span(i):
        kz[i].wait_recv()
        total = kv_y[half_pair, part[i]].astype(F32) + kv_in[part[i]].astype(F32)
        span[part[i]] = total.astype(BF)
        spans[i].start()

    wz.finish()
    wy = RingCopies(
        wg.at[y], lambda i: wg.at[i], lambda i, h: wg.at[i, pl.ds(2 * h, 2)], y, wy_s, wy_r,
        ahead, behind,
    )
    wy.start()

    def told(o, _):
        send(row_ref, rows_got.at[b], row_s.at[o], row_r.at[o], (v, b)).wait_recv()
        return 0

    lax.fori_loop(1, NB, told, 0)
    place[...] = jnp.clip(rows_got[:, 0, :] - 1 - v * TABLE_ROWS, 0, TABLE_ROWS - 1)
    to_scalars = pltpu.make_async_copy(place, place_smem, local.at[1])
    to_scalars.start()
    to_scalars.wait()
    loads[8].wait()

    rings = [
        RingSum(lambda r, h, k=k: chunk.at[k, r, h], y_got.at[k], y_s.at[k], y_r.at[k], ahead, behind)
        for k in range(1, 4)
    ]
    early = [
        RingSum(
            lambda r, h, i=i: chunk.at[0, r, h, part[i]], y_got.at[0, :, part[i]], e_s.at[i],
            e_r.at[i], ahead, behind,
        )
        for i in range(2)
    ]

    def project(k, r):
        for h in range(2):
            peer = lax.rem(y + r, 4) * 4 + lax.rem(z + GROUPS[k][h], 4)

            def eight(i, _, h=h, peer=peer):
                for u in range(8):
                    at = place_smem[peer, 64 * h + i * 8 + u]
                    to = pl.ds(pl.multiple_of(i * 8, 8) + 64 * h + u, 1)
                    rows_f32[to, :] = table_f32[pl.ds(at, 1), :]
                return 0

            lax.fori_loop(0, 8, eight, 0)
        term = jnp.dot(rows_f32[...].astype(BF), inp_ref[...], preferred_element_type=F32)
        chunk[k, r] = term.reshape(2, 64, 896).astype(BF)

    zsum = [
        RingSum(
            lambda r, h, i=i: z_chunk.at[r, h, part[i]], z_got.at[:, part[i]], z_s.at[i],
            z_r.at[i], z_ahead, z_behind,
        )
        for i in range(2)
    ]

    def settle_early(i):
        a, bb = early[i].total()
        z_chunk[2, 0, part[i]] = a.astype(BF)
        z_chunk[2, 1, part[i]] = bb.astype(BF)
        zsum[i].opp_a.start()
        zsum[i].opp_b.start()

    def settle(k):
        a, bb = rings[k - 1].total()
        z_chunk[GROUPS[k][0], 0] = a.astype(BF)
        z_chunk[GROUPS[k][1], 1] = bb.astype(BF)

    def merge(k):
        rings[k - 1].merge_a()
        rings[k - 1].merge_b()

    def go(k, *which):
        for r in which:
            project(k, r)
            open_ring(rings[k - 1], r)

    to_mate = []

    def pass_on(i, src, dst):
        copy = send(src, dst, wc_s.at[i], wc_r.at[i], mate)
        copy.start()
        to_mate.append(copy)

    project(0, 2)
    open_ring(early[0], 2)
    project(0, 1)
    open_ring(early[0], 1)
    open_ring(early[1], 2)
    project(0, 3)
    open_ring(early[0], 3)
    early[0].merge_a()
    early[0].merge_b()
    open_ring(early[1], 1)
    open_ring(early[1], 3)
    project(0, 0)
    early[1].merge_a()
    early[1].merge_b()
    go(1, 2)
    settle_early(0)
    wy.forward()
    go(1, 1)
    settle_early(1)
    go(1, 3)
    share_span(0)

    wy.finish()
    wx = RingCopies(
        wg, lambda i: full.at[c, i], lambda i, h: full.at[c, i, pl.ds(2 * h, 2)], x,
        wx_s, wx_r, x_ahead, x_behind,
    )
    wx.start()
    pass_on(0, wg, full.at[c, x])

    project(2, 2)
    merge(1)
    open_ring(rings[1], 2)
    go(2, 1, 3)
    project(1, 0)
    settle(1)
    for i in range(2):
        zsum[i].next_b.start()
        zsum[i].prev_a.start()
    share_span(1)
    full[c, x] = wg[...]
    project(3, 2)
    merge(2)
    open_ring(rings[2], 2)
    go(3, 1, 3)
    project(2, 0)
    settle(2)
    project(3, 0)
    zsum[0].merge_a()
    zsum[0].merge_b()
    merge(3)
    zsum[1].merge_a()
    zsum[1].merge_b()
    wx.forward()
    for i, o in ((1, 3), (2, 1)):
        slot_ref = full.at[c, lax.rem(x + o, 4)]
        pass_on(i, slot_ref, slot_ref)
    settle(3)
    wx.finish()
    slot_ref = full.at[c, lax.rem(x + 2, 4)]
    pass_on(3, slot_ref, slot_ref)

    for i in range(2):
        a, bb = zsum[i].total()
        sums[0:32] = a
        sums[32:64] = bb
        for h in range(2):
            for q in range(8):
                row = 32 * h + 4 * q
                back_out[16 * h + 8 * i + q] = sums[row : row + 4, :].astype(BF)

        def give(n, _, i=i):
            to = n + 8 * (n // 8) + 8 * i
            o = lax.rem(to - v + NV, NV)

            @pl.when(o != 0)
            def _():
                send(back_out.at[to], back_in.at[v], back_s.at[o], back_r.at[o], (to, b)).start()

            return 0

        lax.fori_loop(0, 16, give, 0)
    back_in[v] = back_out[v]

    for copy in to_mate:
        copy.wait_recv()

    def rows_of(peer, start, count):
        return [
            full[piece % 2, piece // 2, peer // 4, peer % 4, row : row + take, :]
            for _, piece, row, take in packed_rows(start, count)
        ]

    def lay(dst, at, parts, lanes):
        for part in parts:
            dst[at : at + part.shape[0], :] = part[:, lanes]
            at += part.shape[0]

    whole = slice(0, 896)
    for peer in range(NB):
        lay(w_qk, 56 * peer, rows_of(peer, QK_AT, 56), whole)
        for dst, start in ((w_v, V_AT), (w_cq, CQ_AT)):
            parts = rows_of(peer, start, 28)
            lay(dst, 56 * peer, parts, slice(0, 448))
            lay(dst, 56 * peer + 28, parts, slice(448, 896))
        lay(w_so, 28 * peer, rows_of(peer, SO_AT, 28), whole)
        lay(w_co, 28 * peer, rows_of(peer, CO_AT, 28), whole)

    def given(o, _):
        send(back_out.at[v], back_in.at[v], back_s.at[o], back_r.at[o], (v, b)).wait_recv()
        return 0

    lax.fori_loop(1, NV, given, 0)
    for i in range(NV):
        back_rows[4 * i : 4 * i + 4, :] = back_in[i].astype(F32)
    start = jnp.dot(selector[...], back_rows[...].astype(BF), preferred_element_type=F32)
    stream = start.astype(BF).astype(F32)

    self_in = normed(stream, ns_ref[...].reshape(1, 896))
    qk = jnp.dot(self_in, w_qk[...], preferred_element_type=F32).astype(BF)
    vals = jnp.dot(self_in, w_v[...], preferred_element_type=F32).astype(BF)
    heads = attend(qk[:, 0:448], qk[:, 448:896], vals)
    stream = stream + jnp.dot(heads, w_so[...], preferred_element_type=F32)
    cross_in = normed(stream, nc_ref[...].reshape(1, 896))
    cross_q = jnp.dot(cross_in, w_cq[...], preferred_element_type=F32).astype(BF)
    spans[0].wait_recv()
    spans[1].wait_recv()
    span_kv = (span[...].astype(F32) + mate_span[...].astype(F32)).astype(BF)
    heads = attend(cross_q, span_kv[:, 0:448], span_kv[:, 448:896])
    stream = stream + jnp.dot(heads, w_co[...], preferred_element_type=F32)
    out_ref[...] = stream.astype(BF)

    def sent(count, src, dst, ssem, rsem):
        def one(o, _):
            send(src, dst, ssem.at[o], rsem.at[o], (v, b)).wait_send()
            return 0

        lax.fori_loop(1, count, one, 0)

    sent(NV, asks.at[v], ids_got.at[v], ids_s, ids_r)
    sent(NB, row_ref, rows_got.at[b], row_s, row_r)
    sent(NV, back_out.at[v], back_in.at[v], back_s, back_r)
    for ring in (ky, *early, *rings, *zsum, wz, wy, wx):
        ring.drain()
    for copy in (*to_mate, *kz, *spans):
        copy.wait_send()


DMA = pltpu.SemaphoreType.DMA


def body(
    neighbour_ids, query_states, table, in_proj, kv_proj, norm_self, self_qkv, self_out,
    norm_cross, cross_q, cross_out,
):
    vm = pltpu.VMEM
    out = pl.pallas_call(
        kernel,
        out_shape=jax.ShapeDtypeStruct((128, 896), BF),
        in_specs=[pl.BlockSpec(memory_space=vm)] * 3 + [pl.BlockSpec(memory_space=pl.ANY)] * 8,
        out_specs=pl.BlockSpec(memory_space=vm),
        scratch_shapes=[
            vm((4, 128, 256), BF), vm((256, 896), BF), vm((56, 1344), BF), vm((28, 896), BF),
            vm((56, 448), BF), vm((28, 896), BF), vm((256, 896), BF),
            vm((NV, 1, 128), jnp.int32), vm((NV, 1, 128), jnp.int32), vm((1, 128), jnp.int32),
            vm((NB, 1, 128), jnp.int32), vm((NB, 128), jnp.int32), pltpu.SMEM((NB, 128), jnp.int32),
            vm((TABLE_ROWS, 256), BF), vm((TABLE_ROWS, 256), F32), vm((128, 256), F32),
            vm((128, 128), BF),
            vm((8, PIECE, 896), BF), vm((4, 4, PIECE, 896), BF), vm((2, 4, 4, 4, PIECE, 896), BF),
            vm((4, 2, 64, 896), BF), vm((6, 64, 896), BF), vm((2, 64, 896), BF),
            vm((64, 896), BF), vm((64, 896), BF), vm((64, 896), BF),
            vm((4, 4, 2, 64, 896), BF), vm((4, 6, 64, 896), BF), vm((4, 2, 64, 896), BF),
            vm((6, 64, 896), BF), vm((64, 896), F32), vm((NV, 4, 896), BF), vm((NV, 4, 896), BF),
            vm((128, 896), F32),
            vm((896, 896), BF), vm((896, 448), BF), vm((896, 448), BF), vm((448, 896), BF),
            vm((448, 896), BF),
            DMA((9,)), DMA((NV,)), DMA((NV,)), DMA((NB,)), DMA((NB,)),
            DMA((4,)), DMA((4,)), DMA((4,)), DMA((4,)), DMA((4,)), DMA((4,)), DMA((4,)), DMA((4,)),
            DMA((6,)), DMA((6,)), DMA((2,)), DMA((2,)), DMA((2,)), DMA((2,)),
            DMA((2, 6)), DMA((2, 6)), DMA((4, 6)), DMA((4, 6)), DMA((2, 6)), DMA((2, 6)),
            DMA((NV,)), DMA((NV,)),
        ],
        compiler_params=pltpu.CompilerParams(
            collective_id=0, has_side_effects=True, vmem_limit_bytes=VMEM_LIMIT
        ),
        name="encoder",
    )(
        neighbour_ids, norm_self, norm_cross, query_states.reshape(4, 128, 256), kv_proj, self_qkv,
        self_out, cross_q, cross_out, in_proj, table,
    )
    return out.reshape(1, 128, 896)


def solution(mesh):
    both = ("vocab", "batch")
    in_specs = (
        P(both, None), P("vocab", None, "batch"), P("vocab", "batch"), P("batch", None),
        P("batch", None), P(), P("batch", None), P("batch", None), P(), P("batch", None),
        P("batch", None),
    )
    return jax.shard_map(
        body, mesh=mesh, in_specs=in_specs, out_specs=P(both, None, None), check_vma=False
    )
```

```python
import functools

import jax
import jax.numpy as jnp
from jax import lax
from jax.experimental import pallas as pl
from jax.experimental.pallas import tpu as pltpu
from jax.sharding import PartitionSpec as P

MESH = pl.DeviceIdType.MESH
BF = jnp.bfloat16
F32 = jnp.float32
HEAD = 64
NV = 32
NB = 16
QK_AT, V_AT, CQ_AT, SO_AT, CO_AT = 0, 56, 84, 112, 140
PIECE = 24
VMEM_LIMIT = 60 * 1024 * 1024


def where_am_i():
    v = lax.axis_index("vocab")
    b = lax.axis_index("batch")
    return v, b, v // 8, lax.rem(v, 2), b // 4, lax.rem(b, 4)


def send(src, dst, ssem, rsem, dev):
    return pltpu.make_async_remote_copy(
        src_ref=src, dst_ref=dst, send_sem=ssem, recv_sem=rsem,
        device_id=dev, device_id_type=MESH,
    )


def greet(v, b):
    barrier = pltpu.get_barrier_semaphore()

    def hello_vocab(o, _):
        pl.semaphore_signal(
            barrier, inc=1, device_id=(lax.rem(v + o, NV), b), device_id_type=MESH
        )
        return 0

    lax.fori_loop(1, NV, hello_vocab, 0)

    def hello_batch(o, _):
        pl.semaphore_signal(
            barrier, inc=1, device_id=(v, lax.rem(b + o, NB)), device_id_type=MESH
        )
        return 0

    lax.fori_loop(1, NB, hello_batch, 0)


def all_here():
    pl.semaphore_wait(pltpu.get_barrier_semaphore(), NV - 1 + NB - 1)


class RingSum:
    def __init__(self, chunk, got, ssem, rsem, ahead, behind):
        def m(i, src, dev):
            return send(src, got.at[i], ssem.at[i], rsem.at[i], dev)

        self.chunk, self.got = chunk, got
        self.opp_a = m(0, chunk(2, 0), ahead)
        self.opp_b = m(1, chunk(2, 1), behind)
        self.next_b = m(2, chunk(1, 1), ahead)
        self.prev_a = m(3, chunk(3, 0), behind)
        self.merged_a = m(4, chunk(1, 0), ahead)
        self.merged_b = m(5, chunk(3, 1), behind)

    def merge_a(self):
        self.opp_a.wait_recv()
        ref = self.chunk(1, 0)
        ref[...] = (ref[...].astype(F32) + self.got[0].astype(F32)).astype(BF)
        self.merged_a.start()

    def merge_b(self):
        self.opp_b.wait_recv()
        ref = self.chunk(3, 1)
        ref[...] = (ref[...].astype(F32) + self.got[1].astype(F32)).astype(BF)
        self.merged_b.start()

    def total(self):
        self.prev_a.wait_recv()
        self.merged_a.wait_recv()
        a = self.chunk(0, 0)[...].astype(F32) + self.got[3].astype(F32) + self.got[4].astype(F32)
        self.next_b.wait_recv()
        self.merged_b.wait_recv()
        b = self.chunk(0, 1)[...].astype(F32) + self.got[2].astype(F32) + self.got[5].astype(F32)
        return a, b

    def drain(self):
        for c in (self.opp_a, self.opp_b, self.next_b, self.prev_a, self.merged_a, self.merged_b):
            c.wait_send()


class RingCopies:
    def __init__(self, own, slot, half, me, ssem, rsem, ahead, behind):
        left, right = lax.rem(me + 3, 4), lax.rem(me + 1, 4)
        far = lax.rem(me + 2, 4)
        self.to_ahead = send(own, slot(me), ssem.at[0], rsem.at[0], ahead)
        self.to_behind = send(own, slot(me), ssem.at[1], rsem.at[1], behind)
        self.on_ahead = send(half(left, 0), half(left, 0), ssem.at[2], rsem.at[2], ahead)
        self.on_behind = send(half(right, 1), half(right, 1), ssem.at[3], rsem.at[3], behind)
        self.from_left = (slot(left), rsem.at[0])
        self.from_right = (slot(right), rsem.at[1])
        self.far_a = (half(far, 0), rsem.at[2])
        self.far_b = (half(far, 1), rsem.at[3])

    def start(self):
        self.to_ahead.start()
        self.to_behind.start()

    def forward(self):
        self.to_ahead.wait_recv()
        self.on_ahead.start()
        self.to_behind.wait_recv()
        self.on_behind.start()

    def finish(self):
        self.on_ahead.wait_recv()
        self.on_behind.wait_recv()

    def drain(self):
        for c in (self.to_ahead, self.to_behind, self.on_ahead, self.on_behind):
            c.wait_send()


def packed_rows(start, count):
    done = 0
    while done < count:
        at = start + done
        take = min(count - done, PIECE - at % PIECE)
        yield done, at // PIECE, at % PIECE, take
        done += take


def normed(values, gain):
    scale = lax.rsqrt(jnp.mean(values * values, axis=-1, keepdims=True) + 1e-06)
    return (values * scale * gain).astype(BF)


def softmax(scores):
    e = jnp.exp(scores - jnp.max(scores, axis=-1, keepdims=True))
    return (e / jnp.sum(e, axis=-1, keepdims=True)).astype(BF)


def attend(queries, keys, values):
    outs = []
    for h in range(queries.shape[1] // HEAD):
        cut = slice(h * HEAD, (h + 1) * HEAD)
        scores = lax.dot_general(
            queries[:, cut], keys[:, cut], (((1,), (1,)), ((), ())), preferred_element_type=F32
        ) * HEAD ** (-0.5)
        outs.append(jnp.dot(softmax(scores), values[:, cut], preferred_element_type=F32).astype(BF))
    return jnp.concatenate(outs, axis=1)


TABLE_ROWS = 4000
STEP = 160
ORDER = (2, 1, 3, 0)
GROUPS = ((2, 2), (3, 1), (1, 3), (0, 0))


def owner_of(ids):
    return jnp.floor((ids.astype(F32) + 0.5) * (1.0 / TABLE_ROWS)).astype(jnp.int32)


def iota(shape, dim):
    return lax.broadcasted_iota(jnp.int32, shape, dim)


def kernel(
    ids_ref, ns_ref, nc_ref, q_in, kvp_in, qkv_in, so_in, cq_in, co_in, inp_in, table_ref,
    out_ref,
    q_ref, kvp_ref, qkv_ref, so_ref, cq_ref, co_ref, inp_ref,
    asks, ids_got, row_ref, rows_got, place, place_smem, table_bf, table_f32, rows_f32, selector,
    pack, wg, full, kv_chunk, kv_got, kv_y, kv_in, span, mate_span,
    chunk, y_got, z_chunk, z_got, sums, back_out, back_in, back_rows,
    w_qk, w_v, w_cq, w_so, w_co,
    local, ids_s, ids_r, row_s, row_r, wz_s, wz_r, wy_s, wy_r, wx_s, wx_r, wc_s, wc_r,
    ky_s, ky_r, kz_s, kz_r, m_s, m_r, e_s, e_r, y_s, y_r, z_s, z_r, back_s, back_r,
):
    v, b, x, c, y, z = where_am_i()
    greet(v, b)
    rest = lax.rem(v, 8)
    odd = lax.rem(z, 2)
    ahead = (v, lax.rem(y + 1, 4) * 4 + z)
    behind = (v, lax.rem(y + 3, 4) * 4 + z)
    z_ahead = (v, y * 4 + lax.rem(z + 1, 4))
    z_behind = (v, y * 4 + lax.rem(z + 3, 4))
    z_outside = (v, y * 4 + lax.rem(z + 3 + 2 * odd, 4))
    z_mate = (v, y * 4 + z + 1 - 2 * odd)
    x_ahead = (lax.rem(x + 1, 4) * 8 + rest, b)
    x_behind = (lax.rem(x + 3, 4) * 8 + rest, b)
    mate = (v + 1 - 2 * c, b)

    pairs = (
        (table_ref, table_bf), (None, None), (qkv_in, qkv_ref), (so_in, so_ref), (cq_in, cq_ref),
        (co_in, co_ref), (q_in, q_ref), (kvp_in, kvp_ref), (inp_in, inp_ref),
    )
    loads = [
        pltpu.make_async_copy(src, dst, local.at[i]) if src is not None else None
        for i, (src, dst) in enumerate(pairs)
    ]
    for i in (2, 3, 4, 5, 6, 7, 0, 8):
        loads[i].start()

    ids_row = jnp.broadcast_to(ids_ref[...], (128, 128))
    ids_col = ids_row.T
    own_row, own_col = owner_of(ids_row), owner_of(ids_col)
    same = own_row == own_col
    up, across = iota((128, 128), 0), iota((128, 128), 1)
    within_col = jnp.sum(jnp.where(same & (across < up), 1.0, 0.0), axis=1, keepdims=True)
    within_row = jnp.sum(jnp.where(same & (up < across), 1.0, 0.0), axis=0, keepdims=True)
    slot = own_col * 4 + within_col.astype(jnp.int32)
    selector[...] = jnp.where(slot == across, 1.0, 0.0).astype(BF)
    mine = iota((NV, 128), 0) == own_row[:NV]
    lane = iota((NV, 128), 1)
    question = jnp.zeros((NV, 128), jnp.int32)
    for j in range(4):
        hit = mine & (within_row == float(j))
        column = jnp.sum(jnp.where(hit, ids_row[:NV] + 1, 0), axis=1, keepdims=True)
        question = jnp.where(lane == 4 * v + j, column, question)
    asks[...] = question.reshape(NV, 1, 128)

    all_here()

    def ask(o, _):
        to = lax.rem(v + o, NV)
        send(asks.at[to], ids_got.at[v], ids_s.at[o], ids_r.at[o], (to, b)).start()
        return 0

    lax.fori_loop(1, NV, ask, 0)

    ky = RingSum(lambda r, h: kv_chunk.at[r, h], kv_got, ky_s, ky_r, ahead, behind)

    def open_ring(ring, r):
        if r == 2:
            ring.opp_a.start()
            ring.opp_b.start()
        elif r == 1:
            ring.next_b.start()
        elif r == 3:
            ring.prev_a.start()

    loads[6].wait()
    loads[7].wait()
    for r in ORDER:
        term = jnp.dot(q_ref[lax.rem(y + r, 4)], kvp_ref[...], preferred_element_type=F32)
        kv_chunk[r] = term.reshape(2, 64, 896).astype(BF)
        open_ring(ky, r)

    for i in (2, 3, 4, 5):
        loads[i].wait()

    def put(block, start):
        for at, piece, row, take in packed_rows(start, block.shape[0]):
            pack[piece, row : row + take, :] = block[at : at + take]

    put(qkv_ref[:, 0:896], QK_AT)
    put(jnp.concatenate([qkv_ref[0:28, 896:1344], qkv_ref[28:56, 896:1344]], axis=1), V_AT)
    put(jnp.concatenate([cq_ref[0:28, :], cq_ref[28:56, :]], axis=1), CQ_AT)
    put(so_ref[...], SO_AT)
    put(co_ref[...], CO_AT)
    pack[7] = jnp.zeros_like(pack[7])
    wg[y, z] = pack[x * 2 + c]

    wz = RingCopies(
        wg.at[y, z], lambda i: wg.at[y, i], lambda i, h: wg.at[y, i, pl.ds(8 * h, 8 + 8 * h)],
        z, wz_s, wz_r, z_ahead, z_behind,
    )
    wz.start()

    loads[0].wait()

    def widen(i, _):
        at = pl.ds(pl.multiple_of(i * STEP, STEP), STEP)
        table_f32[at, :] = table_bf[at, :].astype(F32)
        return 0

    lax.fori_loop(0, TABLE_ROWS // STEP, widen, 0)

    def asked(o, _):
        send(asks.at[v], ids_got.at[v], ids_s.at[o], ids_r.at[o], (v, b)).wait_recv()
        return 0

    lax.fori_loop(1, NV, asked, 0)
    ids_got[v] = asks[v]
    row_ref[...] = jnp.sum(ids_got[...], axis=0)

    def tell(o, _):
        to = lax.rem(b + o, NB)
        send(row_ref, rows_got.at[b], row_s.at[o], row_r.at[o], (v, to)).start()
        return 0

    lax.fori_loop(1, NB, tell, 0)
    rows_got[b] = row_ref[...]

    ky.merge_a()
    ky.merge_b()
    wz.forward()
    a, bb = ky.total()
    kv_y[0] = a.astype(BF)
    kv_y[1] = bb.astype(BF)
    half_pair = z // 2
    part = [pl.ds(0, 32), pl.ds(32, 32)]
    kz = [
        send(kv_y.at[1 - half_pair, part[i]], kv_in.at[part[i]], kz_s.at[i], kz_r.at[i], z_outside)
        for i in range(2)
    ]
    kz[0].start()
    kz[1].start()
    spans = [
        send(span.at[part[i]], mate_span.at[part[i]], m_s.at[i], m_r.at[i], z_mate)
        for i in range(2)
    ]

    def share_span(i):
        kz[i].wait_recv()
        total = kv_y[half_pair, part[i]].astype(F32) + kv_in[part[i]].astype(F32)
        span[part[i]] = total.astype(BF)
        spans[i].start()

    wz.finish()
    wy = RingCopies(
        wg.at[y], lambda i: wg.at[i], lambda i, h: wg.at[i, pl.ds(2 * h, 2)], y, wy_s, wy_r,
        ahead, behind,
    )
    wy.start()

    def told(o, _):
        send(row_ref, rows_got.at[b], row_s.at[o], row_r.at[o], (v, b)).wait_recv()
        return 0

    lax.fori_loop(1, NB, told, 0)
    place[...] = jnp.clip(rows_got[:, 0, :] - 1 - v * TABLE_ROWS, 0, TABLE_ROWS - 1)
    to_scalars = pltpu.make_async_copy(place, place_smem, local.at[1])
    to_scalars.start()
    to_scalars.wait()
    loads[8].wait()

    rings = [
        RingSum(lambda r, h, k=k: chunk.at[k, r, h], y_got.at[k], y_s.at[k], y_r.at[k], ahead, behind)
        for k in range(1, 4)
    ]
    early = [
        RingSum(
            lambda r, h, i=i: chunk.at[0, r, h, part[i]], y_got.at[0, :, part[i]], e_s.at[i],
            e_r.at[i], ahead, behind,
        )
        for i in range(2)
    ]

    def project(k, r):
        for h in range(2):
            peer = lax.rem(y + r, 4) * 4 + lax.rem(z + GROUPS[k][h], 4)

            def eight(i, _, h=h, peer=peer):
                for u in range(8):
                    at = place_smem[peer, 64 * h + i * 8 + u]
                    to = pl.ds(pl.multiple_of(i * 8, 8) + 64 * h + u, 1)
                    rows_f32[to, :] = table_f32[pl.ds(at, 1), :]
                return 0

            lax.fori_loop(0, 8, eight, 0)
        term = jnp.dot(rows_f32[...].astype(BF), inp_ref[...], preferred_element_type=F32)
        chunk[k, r] = term.reshape(2, 64, 896).astype(BF)

    zsum = [
        RingSum(
            lambda r, h, i=i: z_chunk.at[r, h, part[i]], z_got.at[:, part[i]], z_s.at[i],
            z_r.at[i], z_ahead, z_behind,
        )
        for i in range(2)
    ]

    def settle_early(i):
        a, bb = early[i].total()
        z_chunk[2, 0, part[i]] = a.astype(BF)
        z_chunk[2, 1, part[i]] = bb.astype(BF)
        zsum[i].opp_a.start()
        zsum[i].opp_b.start()

    def settle(k):
        a, bb = rings[k - 1].total()
        z_chunk[GROUPS[k][0], 0] = a.astype(BF)
        z_chunk[GROUPS[k][1], 1] = bb.astype(BF)

    def merge(k):
        rings[k - 1].merge_a()
        rings[k - 1].merge_b()

    def go(k, *which):
        for r in which:
            project(k, r)
            open_ring(rings[k - 1], r)

    to_mate = []

    def pass_on(i, src, dst):
        copy = send(src, dst, wc_s.at[i], wc_r.at[i], mate)
        copy.start()
        to_mate.append(copy)

    project(0, 2)
    open_ring(early[0], 2)
    project(0, 1)
    open_ring(early[0], 1)
    open_ring(early[1], 2)
    project(0, 3)
    open_ring(early[0], 3)
    early[0].merge_a()
    early[0].merge_b()
    open_ring(early[1], 1)
    open_ring(early[1], 3)
    project(0, 0)
    early[1].merge_a()
    early[1].merge_b()
    go(1, 2)
    settle_early(0)
    wy.forward()
    go(1, 1)
    settle_early(1)
    go(1, 3)
    share_span(0)

    wy.finish()
    wx = RingCopies(
        wg, lambda i: full.at[c, i], lambda i, h: full.at[c, i, pl.ds(2 * h, 2)], x,
        wx_s, wx_r, x_ahead, x_behind,
    )
    wx.start()
    pass_on(0, wg, full.at[c, x])

    project(2, 2)
    merge(1)
    open_ring(rings[1], 2)
    go(2, 1, 3)
    project(1, 0)
    settle(1)
    for i in range(2):
        zsum[i].next_b.start()
        zsum[i].prev_a.start()
    share_span(1)
    full[c, x] = wg[...]
    project(3, 2)
    merge(2)
    open_ring(rings[2], 2)
    go(3, 1, 3)
    project(2, 0)
    settle(2)
    project(3, 0)
    zsum[0].merge_a()
    zsum[0].merge_b()
    merge(3)
    zsum[1].merge_a()
    zsum[1].merge_b()
    wx.forward()
    for i, o in ((1, 3), (2, 1)):
        slot_ref = full.at[c, lax.rem(x + o, 4)]
        pass_on(i, slot_ref, slot_ref)
    settle(3)
    wx.finish()
    slot_ref = full.at[c, lax.rem(x + 2, 4)]
    pass_on(3, slot_ref, slot_ref)

    for i in range(2):
        a, bb = zsum[i].total()
        sums[0:32] = a
        sums[32:64] = bb
        for h in range(2):
            for q in range(8):
                row = 32 * h + 4 * q
                back_out[16 * h + 8 * i + q] = sums[row : row + 4, :].astype(BF)

        def give(n, _, i=i):
            to = n + 8 * (n // 8) + 8 * i
            o = lax.rem(to - v + NV, NV)

            @pl.when(o != 0)
            def _():
                send(back_out.at[to], back_in.at[v], back_s.at[o], back_r.at[o], (to, b)).start()

            return 0

        lax.fori_loop(0, 16, give, 0)
    back_in[v] = back_out[v]

    for copy in to_mate:
        copy.wait_recv()

    def rows_of(peer, start, count):
        return [
            full[piece % 2, piece // 2, peer // 4, peer % 4, row : row + take, :]
            for _, piece, row, take in packed_rows(start, count)
        ]

    def lay(dst, at, parts, lanes):
        for part in parts:
            dst[at : at + part.shape[0], :] = part[:, lanes]
            at += part.shape[0]

    whole = slice(0, 896)
    for peer in range(NB):
        lay(w_qk, 56 * peer, rows_of(peer, QK_AT, 56), whole)
        for dst, start in ((w_v, V_AT), (w_cq, CQ_AT)):
            parts = rows_of(peer, start, 28)
            lay(dst, 56 * peer, parts, slice(0, 448))
            lay(dst, 56 * peer + 28, parts, slice(448, 896))
        lay(w_so, 28 * peer, rows_of(peer, SO_AT, 28), whole)
        lay(w_co, 28 * peer, rows_of(peer, CO_AT, 28), whole)

    def given(o, _):
        send(back_out.at[v], back_in.at[v], back_s.at[o], back_r.at[o], (v, b)).wait_recv()
        return 0

    lax.fori_loop(1, NV, given, 0)
    for i in range(NV):
        back_rows[4 * i : 4 * i + 4, :] = back_in[i].astype(F32)
    start = jnp.dot(selector[...], back_rows[...].astype(BF), preferred_element_type=F32)
    stream = start.astype(BF).astype(F32)

    self_in = normed(stream, ns_ref[...].reshape(1, 896))
    qk = jnp.dot(self_in, w_qk[...], preferred_element_type=F32).astype(BF)
    vals = jnp.dot(self_in, w_v[...], preferred_element_type=F32).astype(BF)
    heads = attend(qk[:, 0:448], qk[:, 448:896], vals)
    stream = stream + jnp.dot(heads, w_so[...], preferred_element_type=F32)
    cross_in = normed(stream, nc_ref[...].reshape(1, 896))
    cross_q = jnp.dot(cross_in, w_cq[...], preferred_element_type=F32).astype(BF)
    spans[0].wait_recv()
    spans[1].wait_recv()
    span_kv = (span[...].astype(F32) + mate_span[...].astype(F32)).astype(BF)
    heads = attend(cross_q, span_kv[:, 0:448], span_kv[:, 448:896])
    stream = stream + jnp.dot(heads, w_co[...], preferred_element_type=F32)
    out_ref[...] = stream.astype(BF)

    def sent(count, src, dst, ssem, rsem):
        def one(o, _):
            send(src, dst, ssem.at[o], rsem.at[o], (v, b)).wait_send()
            return 0

        lax.fori_loop(1, count, one, 0)

    sent(NV, asks.at[v], ids_got.at[v], ids_s, ids_r)
    sent(NB, row_ref, rows_got.at[b], row_s, row_r)
    sent(NV, back_out.at[v], back_in.at[v], back_s, back_r)
    for ring in (ky, *early, *rings, *zsum, wz, wy, wx):
        ring.drain()
    for copy in (*to_mate, *kz, *spans):
        copy.wait_send()


DMA = pltpu.SemaphoreType.DMA


def body(
    neighbour_ids, query_states, table, in_proj, kv_proj, norm_self, self_qkv, self_out,
    norm_cross, cross_q, cross_out,
):
    vm = pltpu.VMEM
    out = pl.pallas_call(
        kernel,
        out_shape=jax.ShapeDtypeStruct((128, 896), BF),
        in_specs=[pl.BlockSpec(memory_space=vm)] * 3 + [pl.BlockSpec(memory_space=pl.ANY)] * 8,
        out_specs=pl.BlockSpec(memory_space=vm),
        scratch_shapes=[
            vm((4, 128, 256), BF), vm((256, 896), BF), vm((56, 1344), BF), vm((28, 896), BF),
            vm((56, 448), BF), vm((28, 896), BF), vm((256, 896), BF),
            vm((NV, 1, 128), jnp.int32), vm((NV, 1, 128), jnp.int32), vm((1, 128), jnp.int32),
            vm((NB, 1, 128), jnp.int32), vm((NB, 128), jnp.int32), pltpu.SMEM((NB, 128), jnp.int32),
            vm((TABLE_ROWS, 256), BF), vm((TABLE_ROWS, 256), F32), vm((128, 256), F32),
            vm((128, 128), BF),
            vm((8, PIECE, 896), BF), vm((4, 4, PIECE, 896), BF), vm((2, 4, 4, 4, PIECE, 896), BF),
            vm((4, 2, 64, 896), BF), vm((6, 64, 896), BF), vm((2, 64, 896), BF),
            vm((64, 896), BF), vm((64, 896), BF), vm((64, 896), BF),
            vm((4, 4, 2, 64, 896), BF), vm((4, 6, 64, 896), BF), vm((4, 2, 64, 896), BF),
            vm((6, 64, 896), BF), vm((64, 896), F32), vm((NV, 4, 896), BF), vm((NV, 4, 896), BF),
            vm((128, 896), F32),
            vm((896, 896), BF), vm((896, 448), BF), vm((896, 448), BF), vm((448, 896), BF),
            vm((448, 896), BF),
            DMA((9,)), DMA((NV,)), DMA((NV,)), DMA((NB,)), DMA((NB,)),
            DMA((4,)), DMA((4,)), DMA((4,)), DMA((4,)), DMA((4,)), DMA((4,)), DMA((4,)), DMA((4,)),
            DMA((6,)), DMA((6,)), DMA((2,)), DMA((2,)), DMA((2,)), DMA((2,)),
            DMA((2, 6)), DMA((2, 6)), DMA((4, 6)), DMA((4, 6)), DMA((2, 6)), DMA((2, 6)),
            DMA((NV,)), DMA((NV,)),
        ],
        compiler_params=pltpu.CompilerParams(
            collective_id=0, has_side_effects=True, vmem_limit_bytes=VMEM_LIMIT
        ),
        name="encoder",
    )(
        neighbour_ids, norm_self, norm_cross, query_states.reshape(4, 128, 256), kv_proj, self_qkv,
        self_out, cross_q, cross_out, in_proj, table,
    )
    return out.reshape(1, 128, 896)


def solution(mesh):
    both = ("vocab", "batch")
    in_specs = (
        P(both, None), P("vocab", None, "batch"), P("vocab", "batch"), P("batch", None),
        P("batch", None), P(), P("batch", None), P("batch", None), P(), P("batch", None),
        P("batch", None),
    )
    return jax.shard_map(
        body, mesh=mesh, in_specs=in_specs, out_specs=P(both, None, None), check_vma=False
    )
```
